128 devices in a mesh: row: 8 (over z_lo, y), col: 16 (over x, z_hi, core).
Axes of the slice: x: 4, y: 4, z: 4 (z_hi: 2, z_lo: 2; z = z_hi * 2 + z_lo), core: 2. Of those that a mesh axis runs over, the one named last changes fastest.
Arguments:
- view_a: bfloat16 [12288, 8192], P(('row', 'col')), may hold values from -1000 to 1000
- view_b: bfloat16 [12288, 8192], P(('row', 'col')), may hold values from -1000 to 1000
Outputs:
- correlation: float32 [8192, 8192], P('row', 'col')
- loss: float32 [], replicated
The draws below stay inside these ranges and needn't reach their ends.
All inputs are finite; a program needn't handle non-finite values.
Results may differ from the reference program's by a relative error of at most 0.0013.
Values may be sent and summed in bfloat16 or wider, within the bound.
A program may use at most 192 MiB of HBM per device.

```python
import jax
import jax.numpy as jnp
from jax import lax

D = 8192
TOKENS = 12288


def draw_pair(key):
    keys = jax.random.split(jax.random.fold_in(key, 11), 6)
    ramp = jnp.arange(TOKENS, dtype=jnp.float32) / max(TOKENS - 1, 1)
    row_scale = (1.0 + 2.0 * ramp) * jnp.exp(jax.random.uniform(keys[0], (TOKENS,), jnp.float32, 0.0, jnp.log(3.0)))
    col_scale = jnp.exp(jax.random.uniform(keys[1], (D,), jnp.float32, 0.0, jnp.log(10.0)))
    mixing = jax.random.uniform(keys[2], (D,), jnp.float32, 0.2, 0.95)
    offset = 0.5 * jax.random.normal(keys[3], (D,), jnp.float32)
    base = jax.random.normal(keys[4], (TOKENS, D), jnp.float32)
    noise = jax.random.normal(keys[5], (TOKENS, D), jnp.float32)
    other = mixing * base + jnp.sqrt(1.0 - mixing * mixing) * noise
    scale = row_scale[:, None] * col_scale[None, :]
    first = jnp.clip((base + offset) * scale, -1000.0, 1000.0)
    second = jnp.clip((other + offset) * scale, -1000.0, 1000.0)
    return (first, second)


def draw_view_a(key, part):
    return draw_pair(key)[0].astype(jnp.bfloat16)


def draw_view_b(key, part):
    return draw_pair(key)[1].astype(jnp.bfloat16)


def setup_inputs(seed: int = 0) -> dict:
    seeds = jax.random.split(jax.random.key(seed), 3)
    return {
        "view_a": draw_view_a(jax.random.fold_in(seeds[2], 71), 0),
        "view_b": draw_view_b(jax.random.fold_in(seeds[2], 71), 0),
    }


def normalize(view):
    values = view.astype(jnp.float32)
    count = view.shape[0]
    mean = lax.optimization_barrier(jnp.sum(values, 0)) / count
    var = lax.optimization_barrier(jnp.sum(values * values, 0)) / count - mean * mean
    return ((values - mean) * lax.rsqrt(var + 1e-05)).astype(jnp.bfloat16)

def reference(view_a, view_b):
    norm_a = normalize(view_a).astype(jnp.float32)
    norm_b = normalize(view_b).astype(jnp.float32)
    product = lax.dot_general(norm_a, norm_b, (((0,), (0,)), ((), ())), precision=lax.Precision.HIGHEST, preferred_element_type=jnp.float32)
    correlation = product / view_a.shape[0]
    diag = jnp.diagonal(correlation)
    total = 0.0051 * jnp.sum(correlation * correlation) + jnp.sum((1.0 - diag) ** 2 - 0.0051 * diag * diag)
    loss = total / view_a.shape[1]
    return (correlation, loss)
```

```python
import jax
import jax.numpy as jnp
from jax import lax
from jax.experimental import pallas as pl
from jax.experimental.pallas import tpu as pltpu
from jax.sharding import Mesh
from jax.sharding import PartitionSpec as P

ROW = ("row_0", "row_1")
COL = ("col_0", "col_1", "col_2")
ROW_COL = ("row_0", "row_1", "col_0", "col_1", "col_2")

MESH = pl.DeviceIdType.MESH
F32 = jnp.float32
BF16 = jnp.bfloat16
SENT = BF16

Q = 4
S = 96
AQ = 512
AH = 256
BQ = 256
BH = 128
G = 8
GS = 384
CELLS = Q * Q


def kernel(count, width, a_ref, b_ref, out_ref, loss_ref,
           av, bv, at, bn, psend, pown, precv, prelay,
           ma_mine, ma_in, ma_sum, ma_zin, mb_mine, mb_in, mb_sum, mb_zin, sta, stb,
           lo_mine, lo_in,
           s1a_s, s1a_r, s1b_s, s1b_r,
           aga_s, aga_r, rla_s, rla_r, dd_s, dd_r,
           agb_s, agb_r, rlb_s, rlb_r,
           nr_s, nr_r, fr_s, fr_r, ry_s, ry_r,
           mo_s, mo_r, lo_s, lo_r):
    zl, y, x, zh, c = (lax.axis_index(n) for n in ROW_COL)
    z = zh * 2 + zl

    def dev(x_=None, y_=None, z_=None, c_=None):
        zz = z if z_ is None else z_
        return (lax.rem(zz, 2), y if y_ is None else y_, x if x_ is None else x_,
                lax.div(zz, 2), c if c_ is None else c_)

    def ring(v, d):
        return lax.rem(v + d, 4)

    def xc(r):
        t = lax.rem(x * 2 + c + r, 8)
        return lax.div(t, 2), lax.rem(t, 2)

    def send(src, dst, ss, rs, device):
        cp = pltpu.make_async_remote_copy(src_ref=src, dst_ref=dst, send_sem=ss, recv_sem=rs,
                                          device_id=device, device_id_type=MESH)
        cp.start()

    def wait(ref, sem):
        pltpu.make_async_copy(ref, ref, sem).wait()

    x1, x2, x3 = ring(x, 1), ring(x, 2), ring(x, 3)
    y1, y2, y3 = ring(y, 1), ring(y, 2), ring(y, 3)
    z1, z2, z3 = ring(z, 1), ring(z, 2), ring(z, 3)
    other = 1 - c

    barrier = pltpu.get_barrier_semaphore()
    peers = [dev(y_=v) for v in (y1, y2, y3)] + [dev(z_=v) for v in (z1, z2, z3)]
    for r in range(1, 8):
        px, pc = xc(r)
        peers.append(dev(x_=px, c_=pc))
    for p in peers:
        pl.semaphore_signal(barrier, inc=1, device_id=p, device_id_type=MESH)
    pl.semaphore_wait(barrier, len(peers))

    def stage1(q, carry):
        for d in (1, 3, 2, 0):
            yp = ring(y, d)
            for h in range(2):
                src = a_ref.at[:, pl.ds(pl.multiple_of(h * 4096 + yp * 1024 + q * AH, AH), AH)]
                dst = av.at[q, x, y, c, :, pl.ds(h * AH, AH)]
                if d:
                    send(src, dst, s1a_s, s1a_r.at[q], dev(y_=yp))
                else:
                    pltpu.make_async_copy(src, dst, s1a_r.at[q]).start()
        for r in (1, 2, 3, 7, 6, 5, 4, 0):
            px, pc = xc(r)
            for h in range(2):
                src = b_ref.at[:, pl.ds(pl.multiple_of(px * 2048 + h * 1024 + pc * 512 + q * BH, BH), BH)]
                dst = bv.at[q, x, y, c, :, pl.ds(h * BH, BH)]
                if r:
                    send(src, dst, s1b_s, s1b_r.at[q], dev(x_=px, c_=pc))
                else:
                    pltpu.make_async_copy(src, dst, s1b_r.at[q]).start()
        return carry

    lax.fori_loop(0, Q, stage1, 0)

    def own(q):
        a = av.at[q, x, :, c]
        send(a, a, aga_s.at[q, 0], aga_r.at[q, 0], dev(x_=x1))
        send(a, a, aga_s.at[q, 1], aga_r.at[q, 1], dev(x_=x3))
        b = bv.at[q, :, y]
        send(b, b, agb_s.at[q, 0], agb_r.at[q, 0], dev(y_=y1))
        send(b, b, agb_s.at[q, 1], agb_r.at[q, 1], dev(y_=y3))
        send(a, a, dd_s.at[q, 0], dd_r.at[q, 0], dev(c_=other))

    def own_moments(q, carry):
        def one(k, acc):
            sa, qa, sb, qb = acc
            va = av[q, x, lax.div(k, 2), c, pl.ds(pl.multiple_of(lax.rem(k, 2) * 48, 16), 48), :].astype(F32)
            va = va.reshape(6, 8, AQ)
            sa = sa + jnp.sum(va, 0)
            qa = qa + jnp.sum(va * va, 0)
            vb = bv[q, lax.div(k, 2), y, lax.rem(k, 2)].astype(F32).reshape(12, 8, BQ)
            sb = sb + jnp.sum(vb, 0)
            qb = qb + jnp.sum(vb * vb, 0)
            return sa, qa, sb, qb

        za, zb = jnp.zeros((8, AQ), F32), jnp.zeros((8, BQ), F32)
        sa, qa, sb, qb = lax.fori_loop(0, 8, one, (za, za, zb, zb))
        ma_mine[q, 0:1, :] = jnp.sum(sa, 0, keepdims=True)
        ma_mine[q, 1:2, :] = jnp.sum(qa, 0, keepdims=True)
        mb_mine[q, 0:1, :] = jnp.sum(sb, 0, keepdims=True)
        mb_mine[q, 1:2, :] = jnp.sum(qb, 0, keepdims=True)
        return carry

    def s1_wait(q):
        wait(av.at[q, x, :, c], s1a_r.at[q])
        wait(bv.at[q, :, y], s1b_r.at[q])

    s1_wait(0)
    own(0)
    for q in range(1, Q):
        s1_wait(q)
    lax.fori_loop(0, Q, own_moments, 0)
    for r in range(1, 8):
        px, pc = xc(r)
        send(ma_mine, ma_in.at[r - 1], mo_s.at[0], mo_r.at[0], dev(x_=px, c_=pc))
    for r, v in ((1, y1), (2, y2), (3, y3)):
        send(mb_mine, mb_in.at[r - 1], mo_s.at[1], mo_r.at[1], dev(y_=v))
    own(1)
    wait(ma_in, mo_r.at[0])
    wait(mb_in, mo_r.at[1])
    ma_sum[...] = ma_mine[...] + jnp.sum(ma_in[...], 0)
    mb_sum[...] = mb_mine[...] + jnp.sum(mb_in[...], 0)
    for r, v in ((1, z1), (2, z2), (3, z3)):
        send(ma_sum, ma_zin.at[r - 1], mo_s.at[2], mo_r.at[2], dev(z_=v))
        send(mb_sum, mb_zin.at[r - 1], mo_s.at[3], mo_r.at[3], dev(z_=v))
    wait(ma_zin, mo_r.at[2])
    wait(mb_zin, mo_r.at[3])
    for mine, zin, st in ((ma_sum, ma_zin, sta), (mb_sum, mb_zin, stb)):
        for q in range(Q):
            total = mine[q] + zin[0, q] + zin[1, q] + zin[2, q]
            mean = total[0:1, :] / count
            var = total[1:2, :] / count - mean * mean
            st[q, 0:1, :] = mean
            st[q, 1:2, :] = lax.rsqrt(var + 1e-05)

    def arrive(q):
        wait(av.at[q, x3, :, c], aga_r.at[q, 0])
        a = av.at[q, x3, 0:2, c]
        send(a, a, rla_s.at[q, 0], rla_r.at[q, 0], dev(x_=x1))
        wait(av.at[q, x1, :, c], aga_r.at[q, 1])
        a = av.at[q, x1, 2:4, c]
        send(a, a, rla_s.at[q, 1], rla_r.at[q, 1], dev(x_=x3))
        wait(bv.at[q, :, y3], agb_r.at[q, 0])
        b = bv.at[q, 0:2, y3]
        send(b, b, rlb_s.at[q, 0], rlb_r.at[q, 0], dev(y_=y1))
        wait(bv.at[q, :, y1], agb_r.at[q, 1])
        b = bv.at[q, 2:4, y1]
        send(b, b, rlb_s.at[q, 1], rlb_r.at[q, 1], dev(y_=y3))
        for k, v in ((1, x3), (2, x1)):
            a = av.at[q, v, :, c]
            send(a, a, dd_s.at[q, k], dd_r.at[q, k], dev(c_=other))

    def far(q):
        wait(av.at[q, x2, 0:2, c], rla_r.at[q, 0])
        wait(av.at[q, x2, 2:4, c], rla_r.at[q, 1])
        a = av.at[q, x2, :, c]
        send(a, a, dd_s.at[q, 3], dd_r.at[q, 3], dev(c_=other))
        wait(bv.at[q, 0:2, y2], rlb_r.at[q, 0])
        wait(bv.at[q, 2:4, y2], rlb_r.at[q, 1])
        for k, v in ((0, x), (1, x3), (2, x1), (3, x2)):
            wait(av.at[q, v, :, other], dd_r.at[q, k])

    def normalise(q):
        def group(g, carry):
            x0, yh = lax.div(g, 2), lax.rem(g, 2)
            at_ = pl.multiple_of(g * GS, 128)
            for n in range(AQ // 128):
                cols = pl.ds(n * 128, 128)
                v = av[q, x0, pl.ds(yh * 2, 2), :, :, cols].reshape(GS, 128).astype(F32)
                v = ((v - sta[q, 0:1, cols]) * sta[q, 1:2, cols]).astype(BF16)
                at[q, cols, pl.ds(at_, GS)] = v.T
            for n in range(BQ // 128):
                cols = pl.ds(n * 128, 128)
                v = bv[q, x0, pl.ds(yh * 2, 2), :, :, cols].reshape(GS, 128).astype(F32)
                v = ((v - stb[q, 0:1, cols]) * stb[q, 1:2, cols]).astype(BF16)
                bn[q, pl.ds(at_, GS), cols] = v
            return carry

        lax.fori_loop(0, G, group, 0)

    def multiply(q):
        def cell(t, carry):
            i = jnp.where(t <= q, q, t - q - 1)
            j = jnp.where(t <= q, t, q)
            r = jnp.dot(at[i], bn[j], preferred_element_type=F32) * (1.0 / count)
            for h in range(2):
                for l in range(2):
                    block = r[l * AH:(l + 1) * AH, h * BH:(h + 1) * BH]
                    psend[h * 2 + l, q * q + t] = block.astype(SENT)

                    @pl.when(z == h * 2 + l)
                    def _():
                        pown[q * q + t] = block
            return carry

        lax.fori_loop(0, 2 * q + 1, cell, 0)

    def scatter(q):
        cells = pl.ds(q * q, 2 * q + 1)
        send(psend.at[z2, cells, 0:128], prelay.at[0, cells], fr_s.at[q, 0], fr_r.at[q, 0], dev(z_=z1))
        send(psend.at[z2, cells, 128:256], prelay.at[1, cells], fr_s.at[q, 1], fr_r.at[q, 1], dev(z_=z3))
        send(psend.at[z1, cells], precv.at[0, cells], nr_s.at[q, 0], nr_r.at[q, 0], dev(z_=z1))
        send(psend.at[z3, cells], precv.at[1, cells], nr_s.at[q, 1], nr_r.at[q, 1], dev(z_=z3))

    def pass_on(q):
        cells = pl.ds(q * q, 2 * q + 1)
        wait(prelay.at[0, cells], fr_r.at[q, 0])
        send(prelay.at[0, cells], precv.at[2, cells, 0:128], ry_s.at[q, 0], ry_r.at[q, 0], dev(z_=z1))
        wait(prelay.at[1, cells], fr_r.at[q, 1])
        send(prelay.at[1, cells], precv.at[2, cells, 128:256], ry_s.at[q, 1], ry_r.at[q, 1], dev(z_=z3))

    row0 = (zl * 4 + y) * 1024
    col0 = ((x * 2 + zh) * 2 + c) * 512

    def finish(q):
        cells = pl.ds(q * q, 2 * q + 1)
        wait(precv.at[0, cells], nr_r.at[q, 0])
        wait(precv.at[1, cells], nr_r.at[q, 1])
        wait(precv.at[2, cells, 0:128], ry_r.at[q, 0])
        wait(precv.at[2, cells, 128:256], ry_r.at[q, 1])

        def cell(t, carry):
            i = jnp.where(t <= q, q, t - q - 1)
            j = jnp.where(t <= q, t, q)
            k = q * q + t
            v = (pown[k] + precv[0, k].astype(F32)) + (precv[1, k].astype(F32) + precv[2, k].astype(F32))
            out_ref[pl.ds(pl.multiple_of(i * AH, AH), AH), pl.ds(pl.multiple_of(j * BH, BH), BH)] = v
            rows = row0 + i * AH + lax.broadcasted_iota(jnp.int32, (AH, BH), 0)
            cols = col0 + j * BH + lax.broadcasted_iota(jnp.int32, (AH, BH), 1)
            sq = v * v
            term = jnp.where(rows == cols, (1.0 - v) * (1.0 - v), 0.0051 * sq)
            lo_mine[0] += jnp.sum(term.reshape(AH // 8, 8, BH), 0)
            return carry

        lax.fori_loop(0, 2 * q + 1, cell, 0)

    lo_mine[...] = jnp.zeros_like(lo_mine)
    for q in range(Q):
        arrive(q)
        if q + 2 < Q:
            own(q + 2)
        if q:
            far(q - 1)
            normalise(q - 1)
            multiply(q - 1)
            scatter(q - 1)
            if q > 1:
                pass_on(q - 2)
    far(Q - 1)
    normalise(Q - 1)
    multiply(Q - 1)
    scatter(Q - 1)
    pass_on(Q - 2)
    for q in range(Q - 1):
        finish(q)
    pass_on(Q - 1)
    finish(Q - 1)

    base = 0
    for n, group in enumerate((
        [dev(x_=xc(r)[0], c_=xc(r)[1]) for r in range(1, 8)],
        [dev(y_=v) for v in (y1, y2, y3)],
        [dev(z_=v) for v in (z1, z2, z3)],
    )):
        for k, p in enumerate(group):
            send(lo_mine.at[n], lo_in.at[base + k], lo_s.at[n], lo_r.at[n], p)
        wait(lo_in.at[pl.ds(base, len(group))], lo_r.at[n])
        total = lo_mine[n]
        for k in range(len(group)):
            total = total + lo_in[base + k]
        if n < 2:
            lo_mine[n + 1] = total
        base += len(group)
    loss_ref[0, 0] = jnp.sum(total) / width

    wait(a_ref.at[:, 0:6144], s1a_s)
    wait(b_ref.at[:, 0:7168], s1b_s)
    for q in range(Q):
        for k in range(2):
            wait(av.at[q, x, :, c], aga_s.at[q, k])
            wait(bv.at[q, :, y], agb_s.at[q, k])
            wait(av.at[q, x, 0:2, c], rla_s.at[q, k])
            wait(bv.at[q, 0:2, y], rlb_s.at[q, k])
            cells = pl.ds(q * q, 2 * q + 1)
            wait(precv.at[0, cells], nr_s.at[q, k])
            wait(prelay.at[0, cells], fr_s.at[q, k])
            wait(prelay.at[0, cells], ry_s.at[q, k])
        for k in range(4):
            wait(av.at[q, x, :, c], dd_s.at[q, k])
    wait(ma_in, mo_s.at[0])
    wait(mb_in, mo_s.at[1])
    wait(ma_zin, mo_s.at[2])
    wait(mb_zin, mo_s.at[3])
    wait(lo_in.at[0:7], lo_s.at[0])
    wait(lo_in.at[0:3], lo_s.at[1])
    wait(lo_in.at[0:3], lo_s.at[2])


def shards(view_a, view_b):
    rows, width = view_a.shape
    count = rows * 128
    dma = pltpu.SemaphoreType.DMA
    vm = pltpu.VMEM
    out, loss = pl.pallas_call(
        lambda *refs: kernel(float(count), float(width), *refs),
        out_shape=(jax.ShapeDtypeStruct((1024, 512), F32), jax.ShapeDtypeStruct((1, 1), F32)),
        in_specs=[pl.BlockSpec(memory_space=pl.ANY)] * 2,
        out_specs=(pl.BlockSpec(memory_space=pltpu.VMEM), pl.BlockSpec(memory_space=pltpu.SMEM)),
        scratch_shapes=[
            vm((Q, 4, 4, 2, S, AQ), BF16),
            vm((Q, 4, 4, 2, S, BQ), BF16),
            vm((Q, AQ, G * GS), BF16),
            vm((Q, G * GS, BQ), BF16),
            vm((4, CELLS, AH, BH), SENT),
            vm((CELLS, AH, BH), F32),
            vm((3, CELLS, AH, BH), SENT),
            vm((2, CELLS, AH // 2, BH), SENT),
            vm((Q, 2, AQ), F32), vm((7, Q, 2, AQ), F32), vm((Q, 2, AQ), F32), vm((3, Q, 2, AQ), F32),
            vm((Q, 2, BQ), F32), vm((3, Q, 2, BQ), F32), vm((Q, 2, BQ), F32), vm((3, Q, 2, BQ), F32),
            vm((Q, 2, AQ), F32), vm((Q, 2, BQ), F32),
            vm((3, 8, 128), F32), vm((13, 8, 128), F32),
            dma, dma((Q,)), dma, dma((Q,)),
            dma((Q, 2)), dma((Q, 2)), dma((Q, 2)), dma((Q, 2)), dma((Q, 4)), dma((Q, 4)),
            dma((Q, 2)), dma((Q, 2)), dma((Q, 2)), dma((Q, 2)),
            dma((Q, 2)), dma((Q, 2)), dma((Q, 2)), dma((Q, 2)), dma((Q, 2)), dma((Q, 2)),
            dma((4,)), dma((4,)), dma((3,)), dma((3,)),
        ],
        compiler_params=pltpu.CompilerParams(
            collective_id=0, has_side_effects=True, vmem_limit_bytes=67_000_000),
    )(view_a, view_b)
    return out, loss.reshape(())


def solution(mesh):
    finer = Mesh(mesh.devices.reshape(2, 4, 4, 2, 2), ROW_COL)
    in_specs = (P(ROW_COL, None), P(ROW_COL, None))
    out_specs = (P(ROW, COL), P())
    return jax.shard_map(
        shards, mesh=finer, in_specs=in_specs, out_specs=out_specs, check_vma=False
    )
```

```python
import jax
import jax.numpy as jnp
from jax import lax
from jax.experimental import pallas as pl
from jax.experimental.pallas import tpu as pltpu
from jax.sharding import Mesh
from jax.sharding import PartitionSpec as P

ROW = ("row_0", "row_1")
COL = ("col_0", "col_1", "col_2")
ROW_COL = ("row_0", "row_1", "col_0", "col_1", "col_2")

MESH = pl.DeviceIdType.MESH
F32 = jnp.float32
BF16 = jnp.bfloat16

N = 8
S = 96
AW = 256
BW = 128
GS = 384
K = 3072


def kernel(count, width, a_ref, b_ref, out_ref, loss_ref,
           av, bv, at, bn, psend, precv, prelay,
           ma_mine, ma_in, ma_sum, ma_zin, mb_mine, mb_in, mb_sum, mb_zin, sta, stb,
           lo_sum, lo_mine, lo_in,
           s1a_s, s1a_r, s1b_s, s1b_r,
           aga_s, aga_r, rla_s, rla_r, dd_s, dd_r,
           agb_s, agb_r, rlb_s, rlb_r,
           z1_s, z1_r, z3_s, z3_r, fr_s, fr_r, ry_s, ry_r,
           mo_s, mo_r, lo_s, lo_r):
    zl, y, x, zh, c = (lax.axis_index(n) for n in ROW_COL)

    def scoped(f):
        def g(q, *rest):
            with jax.named_scope(f"{f.__name__}_{q}"):
                return f(q, *rest)
        return g

    def dev(x_=None, y_=None, c_=None, zl_=None, zh_=None):
        return (zl if zl_ is None else zl_, y if y_ is None else y_, x if x_ is None else x_,
                zh if zh_ is None else zh_, c if c_ is None else c_)

    def ring(v, d):
        return lax.rem(v + d, 4)

    def xc(r):
        t = lax.rem(x * 2 + c + r, 8)
        return lax.div(t, 2), lax.rem(t, 2)

    def send(src, dst, ss, rs, device):
        pltpu.make_async_remote_copy(src_ref=src, dst_ref=dst, send_sem=ss, recv_sem=rs,
                                     device_id=device, device_id_type=MESH).start()

    def wait(ref, sem):
        pltpu.make_async_copy(ref, ref, sem).wait()

    x1, x2, x3 = ring(x, 1), ring(x, 2), ring(x, 3)
    y1, y2, y3 = ring(y, 1), ring(y, 2), ring(y, 3)
    other = 1 - c
    p1 = dev(zl_=1 - zl)
    p2 = dev(zh_=1 - zh)
    p3 = dev(zl_=1 - zl, zh_=1 - zh)
    xcs = [dev(x_=xc(r)[0], c_=xc(r)[1]) for r in range(1, 8)]
    ys = [dev(y_=v) for v in (y1, y2, y3)]
    zs = [p1, p2, p3]
    plane = []
    for r in range(1, 32):
        px, pc = xc(r % 8)
        plane.append(dev(x_=px, y_=ring(y, r // 8), c_=pc))

    barrier = pltpu.get_barrier_semaphore()
    peers = xcs + ys + zs
    with jax.named_scope("barrier"):
        for p in peers:
            pl.semaphore_signal(barrier, inc=1, device_id=p, device_id_type=MESH)
        pl.semaphore_wait(barrier, len(peers))

    def stage1(n, carry):
        k = lax.rem(n, 4)
        ha = lax.rem(zl + lax.div(n, 4), 2)
        hb = lax.rem(zh + 1 + lax.div(n, 4), 2)
        for d in (1, 3, 2, 0):
            yp = ring(y, d)
            src = a_ref.at[:, pl.ds(pl.multiple_of(ha * 4096 + yp * 1024 + k * AW, AW), AW)]
            dst = av.at[n, x, y, c]
            if d:
                send(src, dst, s1a_s, s1a_r.at[n], dev(y_=yp))
            else:
                pltpu.make_async_copy(src, dst, s1a_r.at[n]).start()
        for r in (1, 2, 3, 7, 6, 5, 4, 0):
            px, pc = xc(r)
            src = b_ref.at[:, pl.ds(pl.multiple_of(px * 2048 + hb * 1024 + pc * 512 + k * BW, BW), BW)]
            dst = bv.at[n, x, y, c]
            if r:
                send(src, dst, s1b_s, s1b_r.at[n], dev(x_=px, c_=pc))
            else:
                pltpu.make_async_copy(src, dst, s1b_r.at[n]).start()
        return carry

    with jax.named_scope("stage1"):
        lax.fori_loop(0, N, stage1, 0)

    def s1_wait(n):
        wait(av.at[n, x, :, c], s1a_r.at[n])
        wait(bv.at[n, :, y], s1b_r.at[n])

    @scoped
    def own(n, lo=0, hi=4):
        part = pl.ds(lo, hi - lo)
        a = av.at[n, x, part, c]
        send(a, a, aga_s.at[n, 0], aga_r.at[n, 0], dev(x_=x1))
        send(a, a, aga_s.at[n, 1], aga_r.at[n, 1], dev(x_=x3))
        b = bv.at[n, part, y]
        send(b, b, agb_s.at[n, 0], agb_r.at[n, 0], dev(y_=y1))
        send(b, b, agb_s.at[n, 1], agb_r.at[n, 1], dev(y_=y3))
        send(a, a, dd_s.at[n, 0], dd_r.at[n, 0], dev(c_=other))

    def own_moments(n):
        def one(k, acc):
            sa, qa, sb, qb = acc
            va = av[n, x, lax.div(k, 2), c, pl.ds(pl.multiple_of(lax.rem(k, 2) * 48, 16), 48), :].astype(F32)
            va = va.reshape(6, 8, AW)
            sa = sa + jnp.sum(va, 0)
            qa = qa + jnp.sum(va * va, 0)
            vb = bv[n, lax.div(k, 2), y, lax.rem(k, 2)].astype(F32).reshape(12, 8, BW)
            sb = sb + jnp.sum(vb, 0)
            qb = qb + jnp.sum(vb * vb, 0)
            return sa, qa, sb, qb

        za, zb = jnp.zeros((8, AW), F32), jnp.zeros((8, BW), F32)
        sa, qa, sb, qb = lax.fori_loop(0, 8, one, (za, za, zb, zb))
        ma_mine[n, 0:1, :] = jnp.sum(sa, 0, keepdims=True)
        ma_mine[n, 1:2, :] = jnp.sum(qa, 0, keepdims=True)
        mb_mine[n, 0:1, :] = jnp.sum(sb, 0, keepdims=True)
        mb_mine[n, 1:2, :] = jnp.sum(qb, 0, keepdims=True)

    @scoped
    def arrive(n):
        wait(av.at[n, x3, :, c], aga_r.at[n, 0])
        a = av.at[n, x3, 0:2, c]
        send(a, a, rla_s.at[n, 0], rla_r.at[n, 0], dev(x_=x1))
        wait(av.at[n, x1, :, c], aga_r.at[n, 1])
        a = av.at[n, x1, 2:4, c]
        send(a, a, rla_s.at[n, 1], rla_r.at[n, 1], dev(x_=x3))
        wait(bv.at[n, :, y3], agb_r.at[n, 0])
        b = bv.at[n, 0:2, y3]
        send(b, b, rlb_s.at[n, 0], rlb_r.at[n, 0], dev(y_=y1))
        wait(bv.at[n, :, y1], agb_r.at[n, 1])
        b = bv.at[n, 2:4, y1]
        send(b, b, rlb_s.at[n, 1], rlb_r.at[n, 1], dev(y_=y3))
        for k, v in ((1, x3), (2, x1)):
            a = av.at[n, v, :, c]
            send(a, a, dd_s.at[n, k], dd_r.at[n, k], dev(c_=other))

    def wait_and_sum(n, carry):
        s1_wait(n)
        own_moments(n)
        return carry

    with jax.named_scope("s1_wait"):
        s1_wait(0)
        own(0)
        own_moments(0)
        lax.fori_loop(1, N, wait_and_sum, 0)
    for r, p in enumerate(xcs):
        send(ma_mine, ma_in.at[r], mo_s.at[0], mo_r.at[0], p)
    for r, p in enumerate(ys):
        send(mb_mine, mb_in.at[r], mo_s.at[1], mo_r.at[1], p)
    own(1)
    arrive(0)
    own(2)
    with jax.named_scope("mom_1"):
        wait(ma_in, mo_r.at[0])
        wait(mb_in, mo_r.at[1])
    ma_sum[...] = ma_mine[...] + jnp.sum(ma_in[...], 0)
    mb_sum[...] = mb_mine[...] + jnp.sum(mb_in[...], 0)
    for r, p in enumerate(zs):
        send(ma_sum, ma_zin.at[r], mo_s.at[2], mo_r.at[2], p)
        send(mb_sum, mb_zin.at[r], mo_s.at[3], mo_r.at[3], p)
    arrive(1)
    own(3)

    def moments_done():
        with jax.named_scope("mom_2"):
            wait(ma_zin, mo_r.at[2])
            wait(mb_zin, mo_r.at[3])
        for mine, zin, st, turn in ((ma_sum, ma_zin, sta, (4, 0, 4)), (mb_sum, mb_zin, stb, (0, 4, 4))):
            for n in range(N):
                total = mine[n] + zin[0, (n + turn[0]) % N] + zin[1, (n + turn[1]) % N] + zin[2, (n + turn[2]) % N]
                mean = total[0:1, :] / count
                var = total[1:2, :] / count - mean * mean
                st[n, 0:1, :] = mean
                st[n, 1:2, :] = lax.rsqrt(var + 1e-05)

    @scoped
    def far(n):
        wait(av.at[n, x2, 0:2, c], rla_r.at[n, 0])
        wait(av.at[n, x2, 2:4, c], rla_r.at[n, 1])
        a = av.at[n, x2, :, c]
        send(a, a, dd_s.at[n, 3], dd_r.at[n, 3], dev(c_=other))
        wait(bv.at[n, 0:2, y2], rlb_r.at[n, 0])
        wait(bv.at[n, 2:4, y2], rlb_r.at[n, 1])

    def norm_a(n, lo, hi):
        def group(g, carry):
            x0, yh = ring(x2 + 1, lax.div(g, 2)), lax.rem(g, 2)
            at_ = pl.multiple_of((x0 * 2 + yh) * GS, 128)
            for m in range(AW // 128):
                cols = pl.ds(m * 128, 128)
                v = av[n, x0, pl.ds(yh * 2, 2), :, :, cols].reshape(GS, 128).astype(F32)
                v = ((v - sta[n, 0:1, cols]) * sta[n, 1:2, cols]).astype(BF16)
                at[n, cols, pl.ds(at_, GS)] = v.T
            return carry

        lax.fori_loop(lo, hi, group, 0)

    def norm_b(n, lo, hi):
        cols = pl.ds((n % 4) * BW, BW)

        def group(g, carry):
            x0, yh = lax.rem(g, 4), lax.rem(lax.div(y2, 2) + 1 + lax.div(g, 4), 2)
            at_ = pl.multiple_of((x0 * 2 + yh) * GS, 128)
            v = bv[n, x0, pl.ds(yh * 2, 2)].reshape(GS, BW).astype(F32)
            v = ((v - stb[n, 0:1, :]) * stb[n, 1:2, :]).astype(BF16)
            bn[n // 4, pl.ds(at_, GS), cols] = v
            return carry

        lax.fori_loop(lo, hi, group, 0)

    @scoped
    def near_norm(n):
        for k, v in ((0, x), (1, x3), (2, x1)):
            wait(av.at[n, v, :, other], dd_r.at[n, k])
        norm_a(n, 0, 6)
        norm_b(n, 0, 4)

    @scoped
    def far_norm(n):
        wait(av.at[n, x2, :, other], dd_r.at[n, 3])
        norm_a(n, 6, 8)
        norm_b(n, 4, 8)

    def dot(i, half, j, n):
        r = jnp.dot(at[i], bn[half, :, j * BW:(j + n) * BW], preferred_element_type=F32)
        return r * (1.0 / count)

    def row(slot, m, i, half, n):
        r = dot(i, half, 0, n)
        for j in range(n):
            psend[slot, m, j] = r[:, j * BW:(j + 1) * BW].astype(BF16)

    def column(slot, m, base, half):
        def one(i, carry):
            psend[slot, i, m] = dot(base + i, half, m, 1).astype(BF16)
            return carry

        lax.fori_loop(0, m, one, 0)

    def parts(m):
        yield 0, (m, pl.ds(0, m + 1))
        if m:
            yield 1, (pl.ds(0, m), m)

    HALVES = ((0, pl.ds(0, 128)), (1, pl.ds(128, 128)))

    @scoped
    def multiply_far(m):
        row(1, m, m, 0, m + 1)
        column(1, m, 0, 0)
        for k, cells in parts(m):
            for h, rows in HALVES:
                send(psend.at[(1, *cells, rows)], prelay.at[(h, *cells)],
                     fr_s.at[m, k, h], fr_r.at[m, k, h], (p1, p3)[h])

    def send_1(m, k):
        for kk, cells in parts(m):
            if kk == k:
                send(psend.at[(0, *cells)], precv.at[(0, *cells)], z1_s.at[m, k], z1_r.at[m, k], p1)

    @scoped
    def row_1(n):
        row(0, n - 4, n, 1, n - 3)
        send_1(n - 4, 0)

    @scoped
    def column_1(n):
        column(0, n - 4, 4, 1)
        send_1(n - 4, 1)

    @scoped
    def multiply_3(n):
        m = n % 4
        row(2, m, n, 0, 4)
        send(psend.at[2, m], precv.at[2, m], z3_s.at[m], z3_r.at[m], p3)

    @scoped
    def pass_on(m):
        for k, cells in parts(m):
            for h, rows in HALVES:
                src = prelay.at[(h, *cells)]
                wait(src, fr_r.at[m, k, h])
                send(src, precv.at[(1, *cells, rows)], ry_s.at[m, k, h], ry_r.at[m, k, h], (p3, p1)[h])

    row0 = (zl * 4 + y) * 1024
    col0 = ((x * 2 + zh) * 2 + c) * 512

    def finish(i, j):
        at_ = (pl.ds(pl.multiple_of(i * AW, AW), AW), pl.ds(pl.multiple_of(j * BW, BW), BW))
        v = out_ref[at_] + precv[1, i, j].astype(F32) + precv[2, i, j].astype(F32) + precv[0, i, j].astype(F32)
        out_ref[at_] = v
        rows = row0 + i * AW + lax.broadcasted_iota(jnp.int32, (AW, BW), 0)
        cols = col0 + j * BW + lax.broadcasted_iota(jnp.int32, (AW, BW), 1)
        term = jnp.where(rows == cols, (1.0 - v) * (1.0 - v), 0.0051 * (v * v))
        lo_sum[...] += jnp.sum(term.reshape(AW // 8, 8, BW), 0)

    lo_sum[...] = jnp.zeros_like(lo_sum)
    moments_done()
    for n in range(1, N - 1):
        if n > 1:
            arrive(n)
            if n + 2 < N - 1:
                own(n + 2)
            elif n + 2 == N - 1:
                own(N - 1, 0, 2)
            else:
                own(N - 1, 2, 4)
        near_norm(n - 1)
        far(n - 1)
        if n == 6:
            pass_on(3)
        far_norm(n - 1)
        if n < 5:
            multiply_far(n - 1)
        else:
            row_1(n - 1)
            column_1(n - 1)
            multiply_3(n - 1)
        if 2 <= n < 5:
            pass_on(n - 2)
    near_norm(N - 2)
    far(N - 2)
    arrive(N - 1)
    far_norm(N - 2)
    row_1(N - 2)
    far(N - 1)
    column_1(N - 2)
    near_norm(N - 1)
    far_norm(N - 1)
    multiply_3(N - 2)
    row_1(N - 1)
    column_1(N - 1)
    multiply_3(N - 1)

    with jax.named_scope("mine"):
        def mine(i, carry):
            out_ref[pl.ds(pl.multiple_of(i * AW, AW), AW), :] = dot(i, 1, 0, 4)
            return carry

        lax.fori_loop(0, 4, mine, 0)

    def z1_wait(m):
        for k, cells in parts(m):
            wait(precv.at[(0, *cells)], z1_r.at[m, k])

    with jax.named_scope("finish_early"):
        for m in range(4):
            for k, cells in parts(m):
                for h, rows in HALVES:
                    wait(precv.at[(1, *cells, rows)], ry_r.at[m, k, h])
        for m in range(3):
            wait(precv.at[2, m], z3_r.at[m])
            z1_wait(m)

        def early(t, carry):
            finish(lax.div(t, 3), lax.rem(t, 3))
            return carry

        lax.fori_loop(0, 9, early, 0)
    with jax.named_scope("finish_late"):
        wait(precv.at[2, 3], z3_r.at[3])
        z1_wait(3)

        def late(t, carry):
            finish(jnp.where(t < 4, 3, t - 4), jnp.where(t < 4, t, 3))
            return carry

        lax.fori_loop(0, 7, late, 0)

    lo_mine[0] = jnp.sum(lo_sum[...], 0, keepdims=True)
    base = 0
    for k, group in enumerate((plane, zs)):
        for r, p in enumerate(group):
            send(lo_mine.at[k], lo_in.at[base + r], lo_s.at[k], lo_r.at[k], p)
        with jax.named_scope(f"loss_{k}"):
            wait(lo_in.at[pl.ds(base, len(group))], lo_r.at[k])
        total = lo_mine[k] + jnp.sum(lo_in[pl.ds(base, len(group))], 0)
        if k == 0:
            lo_mine[1] = total
        base += len(group)
    loss_ref[0, 0] = jnp.sum(total) / width

    with jax.named_scope("drain"):
        wait(a_ref.at[:, 0:6144], s1a_s)
        wait(b_ref.at[:, 0:7168], s1b_s)
        for n in range(N):
            for k in range(2):
                wait(av.at[n, x, :, c], aga_s.at[n, k])
                wait(bv.at[n, :, y], agb_s.at[n, k])
                wait(av.at[n, x, 0:2, c], rla_s.at[n, k])
                wait(bv.at[n, 0:2, y], rlb_s.at[n, k])
            for k in range(4):
                wait(av.at[n, x, :, c], dd_s.at[n, k])
        for m in range(4):
            for k, cells in parts(m):
                wait(precv.at[(0, *cells)], z1_s.at[m, k])
                for h, rows in HALVES:
                    wait(prelay.at[(h, *cells)], fr_s.at[m, k, h])
                    wait(prelay.at[(h, *cells)], ry_s.at[m, k, h])
            wait(precv.at[2, m], z3_s.at[m])
        wait(ma_in, mo_s.at[0])
        wait(mb_in, mo_s.at[1])
        wait(ma_zin, mo_s.at[2])
        wait(mb_zin, mo_s.at[3])
        wait(lo_in.at[0:31], lo_s.at[0])
        wait(lo_in.at[0:3], lo_s.at[1])


def shards(view_a, view_b):
    rows, width = view_a.shape
    count = rows * 128
    dma = pltpu.SemaphoreType.DMA
    vm = pltpu.VMEM
    out, loss = pl.pallas_call(
        lambda *refs: kernel(float(count), float(width), *refs),
        out_shape=(pltpu.VMEM((1024, 512), F32), jax.ShapeDtypeStruct((1, 1), F32)),
        in_specs=[pl.BlockSpec(memory_space=pl.ANY)] * 2,
        out_specs=(pl.BlockSpec(memory_space=pltpu.VMEM), pl.BlockSpec(memory_space=pltpu.SMEM)),
        scratch_shapes=[
            vm((N, 4, 4, 2, S, AW), BF16),
            vm((N, 4, 4, 2, S, BW), BF16),
            vm((N, AW, K), BF16),
            vm((2, K, 4 * BW), BF16),
            vm((3, 4, 4, AW, BW), BF16),
            vm((3, 4, 4, AW, BW), BF16),
            vm((2, 4, 4, AW // 2, BW), BF16),
            vm((N, 2, AW), F32), vm((7, N, 2, AW), F32), vm((N, 2, AW), F32), vm((3, N, 2, AW), F32),
            vm((N, 2, BW), F32), vm((3, N, 2, BW), F32), vm((N, 2, BW), F32), vm((3, N, 2, BW), F32),
            vm((N, 2, AW), F32), vm((N, 2, BW), F32),
            vm((8, 128), F32), vm((2, 1, 128), F32), vm((34, 1, 128), F32),
            dma, dma((N,)), dma, dma((N,)),
            dma((N, 2)), dma((N, 2)), dma((N, 2)), dma((N, 2)), dma((N, 4)), dma((N, 4)),
            dma((N, 2)), dma((N, 2)), dma((N, 2)), dma((N, 2)),
            dma((4, 2)), dma((4, 2)), dma((4,)), dma((4,)),
            dma((4, 2, 2)), dma((4, 2, 2)), dma((4, 2, 2)), dma((4, 2, 2)),
            dma((4,)), dma((4,)), dma((2,)), dma((2,)),
        ],
        compiler_params=pltpu.CompilerParams(
            collective_id=0, has_side_effects=True, vmem_limit_bytes=56_000_000),
    )(view_a, view_b)
    return out, loss.reshape(())


def solution(mesh):
    finer = Mesh(mesh.devices.reshape(2, 4, 4, 2, 2), ROW_COL)
    in_specs = (P(ROW_COL, None), P(ROW_COL, None))
    out_specs = (P(ROW, COL), P())
    return jax.shard_map(
        shards, mesh=finer, in_specs=in_specs, out_specs=out_specs, check_vma=False
    )
```

```python
import jax
import jax.numpy as jnp
from jax import lax
from jax.experimental import pallas as pl
from jax.experimental.pallas import tpu as pltpu
from jax.sharding import Mesh
from jax.sharding import PartitionSpec as P

ROW = ("row_0", "row_1")
COL = ("col_0", "col_1", "col_2")
ROW_COL = ("row_0", "row_1", "col_0", "col_1", "col_2")

MESH = pl.DeviceIdType.MESH
F32 = jnp.float32
BF16 = jnp.bfloat16

N = 8
S = 96
AW = 256
BW = 128
GS = 384
K = 3072


def kernel(count, width, a_hbm, b_hbm, out_ref, loss_ref,
           a_ref, b_ref, in_s, av, bv, at, bn, psend, precv, prelay,
           ma_mine, ma_in, ma_sum, ma_zin, mb_mine, mb_in, mb_sum, mb_zin, sta, stb,
           lo_sum, lo_mine, lo_in,
           s1a_s, s1a_r, s1b_s, s1b_r,
           aga_s, aga_r, rla_s, rla_r, dd_s, dd_r,
           agb_s, agb_r, rlb_s, rlb_r,
           z1_s, z1_r, z3_s, z3_r, fr_s, fr_r, ry_s, ry_r,
           mo_s, mo_r, lo_s, lo_r):
    zl, y, x, zh, c = (lax.axis_index(n) for n in ROW_COL)

    def scoped(f):
        def g(q, *rest):
            with jax.named_scope(f"{f.__name__}_{q}"):
                return f(q, *rest)
        return g

    def dev(x_=None, y_=None, c_=None, zl_=None, zh_=None):
        return (zl if zl_ is None else zl_, y if y_ is None else y_, x if x_ is None else x_,
                zh if zh_ is None else zh_, c if c_ is None else c_)

    def ring(v, d):
        return lax.rem(v + d, 4)

    def xc(r):
        t = lax.rem(x * 2 + c + r, 8)
        return lax.div(t, 2), lax.rem(t, 2)

    def send(src, dst, ss, rs, device):
        pltpu.make_async_remote_copy(src_ref=src, dst_ref=dst, send_sem=ss, recv_sem=rs,
                                     device_id=device, device_id_type=MESH).start()

    def wait(ref, sem):
        pltpu.make_async_copy(ref, ref, sem).wait()

    x1, x2, x3 = ring(x, 1), ring(x, 2), ring(x, 3)
    y1, y2, y3 = ring(y, 1), ring(y, 2), ring(y, 3)
    other = 1 - c
    p1 = dev(zl_=1 - zl)
    p2 = dev(zh_=1 - zh)
    p3 = dev(zl_=1 - zl, zh_=1 - zh)
    xcs = [dev(x_=xc(r)[0], c_=xc(r)[1]) for r in range(1, 8)]
    ys = [dev(y_=v) for v in (y1, y2, y3)]
    zs = [p1, p2, p3]
    load_a = pltpu.make_async_copy(a_hbm, a_ref, in_s.at[0])
    load_b = pltpu.make_async_copy(b_hbm, b_ref, in_s.at[1])
    load_a.start()
    load_b.start()

    barrier = pltpu.get_barrier_semaphore()
    peers = xcs + ys + zs
    with jax.named_scope("barrier"):
        for p in peers:
            pl.semaphore_signal(barrier, inc=1, device_id=p, device_id_type=MESH)
        pl.semaphore_wait(barrier, len(peers))
    load_a.wait()
    load_b.wait()

    def stage1(n, carry):
        k = lax.rem(n, 4)
        ha = lax.rem(zl + lax.div(n, 4), 2)
        hb = lax.rem(zh + 1 + lax.div(n, 4), 2)
        for d in (1, 3, 2, 0):
            yp = ring(y, d)
            cols = pl.ds(pl.multiple_of(ha * 4096 + yp * 1024 + k * AW, AW), AW)
            dst = av.at[n, x, y, c]
            if d:
                send(a_ref.at[:, cols], dst, s1a_s, s1a_r.at[n], dev(y_=yp))
            else:
                pltpu.make_async_copy(a_hbm.at[:, cols], dst, s1a_r.at[n]).start()
        for r in (1, 2, 3, 7, 6, 5, 4, 0):
            px, pc = xc(r)
            cols = pl.ds(pl.multiple_of(px * 2048 + hb * 1024 + pc * 512 + k * BW, BW), BW)
            dst = bv.at[n, x, y, c]
            if r:
                send(b_ref.at[:, cols], dst, s1b_s, s1b_r.at[n], dev(x_=px, c_=pc))
            else:
                pltpu.make_async_copy(b_hbm.at[:, cols], dst, s1b_r.at[n]).start()
        return carry

    with jax.named_scope("stage1"):
        lax.fori_loop(0, N, stage1, 0)

    def s1_wait(n):
        wait(av.at[n, x, :, c], s1a_r.at[n])
        wait(bv.at[n, :, y], s1b_r.at[n])

    @scoped
    def own(n, lo=0, hi=4):
        part = pl.ds(lo, hi - lo)
        a = av.at[n, x, part, c]
        send(a, a, aga_s.at[n, 0], aga_r.at[n, 0], dev(x_=x1))
        send(a, a, aga_s.at[n, 1], aga_r.at[n, 1], dev(x_=x3))
        b = bv.at[n, part, y]
        send(b, b, agb_s.at[n, 0], agb_r.at[n, 0], dev(y_=y1))
        send(b, b, agb_s.at[n, 1], agb_r.at[n, 1], dev(y_=y3))
        send(a, a, dd_s.at[n, 0], dd_r.at[n, 0], dev(c_=other))

    def own_moments(n):
        def one(k, acc):
            sa, qa, sb, qb = acc
            va = av[n, x, lax.div(k, 2), c, pl.ds(pl.multiple_of(lax.rem(k, 2) * 48, 16), 48), :].astype(F32)
            va = va.reshape(6, 8, AW)
            sa = sa + jnp.sum(va, 0)
            qa = qa + jnp.sum(va * va, 0)
            vb = bv[n, lax.div(k, 2), y, lax.rem(k, 2)].astype(F32).reshape(12, 8, BW)
            sb = sb + jnp.sum(vb, 0)
            qb = qb + jnp.sum(vb * vb, 0)
            return sa, qa, sb, qb

        za, zb = jnp.zeros((8, AW), F32), jnp.zeros((8, BW), F32)
        sa, qa, sb, qb = lax.fori_loop(0, 8, one, (za, za, zb, zb))
        ma_mine[n, 0:1, :] = jnp.sum(sa, 0, keepdims=True)
        ma_mine[n, 1:2, :] = jnp.sum(qa, 0, keepdims=True)
        mb_mine[n, 0:1, :] = jnp.sum(sb, 0, keepdims=True)
        mb_mine[n, 1:2, :] = jnp.sum(qb, 0, keepdims=True)

    @scoped
    def arrive(n):
        wait(av.at[n, x3, :, c], aga_r.at[n, 0])
        a = av.at[n, x3, 0:2, c]
        send(a, a, rla_s.at[n, 0], rla_r.at[n, 0], dev(x_=x1))
        wait(av.at[n, x1, :, c], aga_r.at[n, 1])
        a = av.at[n, x1, 2:4, c]
        send(a, a, rla_s.at[n, 1], rla_r.at[n, 1], dev(x_=x3))
        wait(bv.at[n, :, y3], agb_r.at[n, 0])
        b = bv.at[n, 0:2, y3]
        send(b, b, rlb_s.at[n, 0], rlb_r.at[n, 0], dev(y_=y1))
        wait(bv.at[n, :, y1], agb_r.at[n, 1])
        b = bv.at[n, 2:4, y1]
        send(b, b, rlb_s.at[n, 1], rlb_r.at[n, 1], dev(y_=y3))
        for k, v in ((1, x3), (2, x1)):
            a = av.at[n, v, :, c]
            send(a, a, dd_s.at[n, k], dd_r.at[n, k], dev(c_=other))

    def wait_and_sum(n, carry):
        s1_wait(n)
        own_moments(n)
        return carry

    with jax.named_scope("s1_wait"):
        s1_wait(0)
        own(0)
        own_moments(0)
        lax.fori_loop(1, N, wait_and_sum, 0)
    for r, p in enumerate(xcs):
        send(ma_mine, ma_in.at[r], mo_s.at[0], mo_r.at[0], p)
    for r, p in enumerate(ys):
        send(mb_mine, mb_in.at[r], mo_s.at[1], mo_r.at[1], p)
    own(1)
    arrive(0)
    own(2)
    with jax.named_scope("mom_1"):
        wait(ma_in, mo_r.at[0])
        wait(mb_in, mo_r.at[1])
    ma_sum[...] = ma_mine[...] + jnp.sum(ma_in[...], 0)
    mb_sum[...] = mb_mine[...] + jnp.sum(mb_in[...], 0)
    for r, p in enumerate(zs):
        send(ma_sum, ma_zin.at[r], mo_s.at[2], mo_r.at[2], p)
        send(mb_sum, mb_zin.at[r], mo_s.at[3], mo_r.at[3], p)
    arrive(1)
    own(3)

    def moments_done():
        with jax.named_scope("mom_2"):
            wait(ma_zin, mo_r.at[2])
            wait(mb_zin, mo_r.at[3])
        for mine, zin, st, turn in ((ma_sum, ma_zin, sta, (4, 0, 4)), (mb_sum, mb_zin, stb, (0, 4, 4))):
            for n in range(N):
                total = mine[n] + zin[0, (n + turn[0]) % N] + zin[1, (n + turn[1]) % N] + zin[2, (n + turn[2]) % N]
                mean = total[0:1, :] / count
                var = total[1:2, :] / count - mean * mean
                st[n, 0:1, :] = mean
                st[n, 1:2, :] = lax.rsqrt(var + 1e-05)

    @scoped
    def far(n):
        wait(av.at[n, x2, 0:2, c], rla_r.at[n, 0])
        wait(av.at[n, x2, 2:4, c], rla_r.at[n, 1])
        a = av.at[n, x2, :, c]
        send(a, a, dd_s.at[n, 3], dd_r.at[n, 3], dev(c_=other))
        wait(bv.at[n, 0:2, y2], rlb_r.at[n, 0])
        wait(bv.at[n, 2:4, y2], rlb_r.at[n, 1])

    def norm_a(n, lo, hi):
        def group(g, carry):
            x0, yh = ring(x2 + 1, lax.div(g, 2)), lax.rem(g, 2)
            at_ = pl.multiple_of((x0 * 2 + yh) * GS, 128)
            for m in range(AW // 128):
                cols = pl.ds(m * 128, 128)
                v = av[n, x0, pl.ds(yh * 2, 2), :, :, cols].reshape(GS, 128).astype(F32)
                v = ((v - sta[n, 0:1, cols]) * sta[n, 1:2, cols]).astype(BF16)
                at[n, cols, pl.ds(at_, GS)] = v.T
            return carry

        lax.fori_loop(lo, hi, group, 0)

    def norm_b(n, lo, hi):
        cols = pl.ds((n % 4) * BW, BW)

        def group(g, carry):
            x0, yh = lax.rem(g, 4), lax.rem(lax.div(y2, 2) + 1 + lax.div(g, 4), 2)
            at_ = pl.multiple_of((x0 * 2 + yh) * GS, 128)
            v = bv[n, x0, pl.ds(yh * 2, 2)].reshape(GS, BW).astype(F32)
            v = ((v - stb[n, 0:1, :]) * stb[n, 1:2, :]).astype(BF16)
            bn[n // 4, pl.ds(at_, GS), cols] = v
            return carry

        lax.fori_loop(lo, hi, group, 0)

    @scoped
    def near_norm(n):
        for k, v in ((0, x), (1, x3), (2, x1)):
            wait(av.at[n, v, :, other], dd_r.at[n, k])
        norm_a(n, 0, 6)
        norm_b(n, 0, 4)

    @scoped
    def far_norm(n):
        wait(av.at[n, x2, :, other], dd_r.at[n, 3])
        norm_a(n, 6, 8)
        norm_b(n, 4, 8)

    def dot(i, half, j, n):
        r = jnp.dot(at[i], bn[half, :, j * BW:(j + n) * BW], preferred_element_type=F32)
        return r * (1.0 / count)

    def row(slot, m, i, half, n):
        r = dot(i, half, 0, n)
        for j in range(n):
            psend[slot, m, j] = r[:, j * BW:(j + 1) * BW].astype(BF16)

    def column(slot, m, base, half):
        def one(i, carry):
            psend[slot, i, m] = dot(base + i, half, m, 1).astype(BF16)
            return carry

        lax.fori_loop(0, m, one, 0)

    def parts(m):
        yield 0, (m, pl.ds(0, m + 1))
        if m:
            yield 1, (pl.ds(0, m), m)

    HALVES = ((0, pl.ds(0, 128)), (1, pl.ds(128, 128)))

    @scoped
    def pass_on(m):
        for k, cells in parts(m):
            for h, rows in HALVES:
                src = prelay.at[(h, *cells)]
                wait(src, fr_r.at[m, k, h])
                send(src, precv.at[(1, *cells, rows)], ry_s.at[m, k, h], ry_r.at[m, k, h], (p3, p1)[h])

    @scoped
    def multiply_far(m):
        row(1, m, m, 0, m + 1)
        if m:
            pass_on(m - 1)
        column(1, m, 0, 0)
        for k, cells in parts(m):
            for h, rows in HALVES:
                send(psend.at[(1, *cells, rows)], prelay.at[(h, *cells)],
                     fr_s.at[m, k, h], fr_r.at[m, k, h], (p1, p3)[h])

    def send_1(m, k):
        for kk, cells in parts(m):
            if kk == k:
                send(psend.at[(0, *cells)], precv.at[(0, *cells)], z1_s.at[m, k], z1_r.at[m, k], p1)

    @scoped
    def row_1(n):
        row(0, n - 4, n, 1, n - 3)
        send_1(n - 4, 0)

    @scoped
    def column_1(n):
        column(0, n - 4, 4, 1)
        send_1(n - 4, 1)

    @scoped
    def multiply_3(n):
        m = n % 4
        row(2, m, n, 0, 4)
        send(psend.at[2, m], precv.at[2, m], z3_s.at[m], z3_r.at[m], p3)

    row0 = (zl * 4 + y) * 1024
    col0 = ((x * 2 + zh) * 2 + c) * 512

    def finish(i, j):
        at_ = (pl.ds(pl.multiple_of(i * AW, AW), AW), pl.ds(pl.multiple_of(j * BW, BW), BW))
        v = out_ref[at_] + precv[1, i, j].astype(F32) + precv[2, i, j].astype(F32) + precv[0, i, j].astype(F32)
        out_ref[at_] = v
        rows = row0 + i * AW + lax.broadcasted_iota(jnp.int32, (AW, BW), 0)
        cols = col0 + j * BW + lax.broadcasted_iota(jnp.int32, (AW, BW), 1)
        term = jnp.where(rows == cols, (1.0 - v) * (1.0 - v), 0.0051 * (v * v))
        lo_sum[...] += jnp.sum(term.reshape(AW // 8, 8, BW), 0)

    lo_sum[...] = jnp.zeros_like(lo_sum)
    moments_done()
    for n in range(1, N - 1):
        if n > 1:
            arrive(n)
            if n + 2 < N - 1:
                own(n + 2)
            elif n + 2 == N - 1:
                own(N - 1, 0, 2)
            else:
                own(N - 1, 2, 4)
        near_norm(n - 1)
        far(n - 1)
        if n == 6:
            pass_on(3)
        far_norm(n - 1)
        if n < 5:
            multiply_far(n - 1)
        else:
            row_1(n - 1)
            column_1(n - 1)
            multiply_3(n - 1)
    near_norm(N - 2)
    far(N - 2)
    arrive(N - 1)
    far_norm(N - 2)
    row_1(N - 2)
    far(N - 1)
    column_1(N - 2)
    near_norm(N - 1)
    far_norm(N - 1)
    multiply_3(N - 2)
    row_1(N - 1)
    column_1(N - 1)
    multiply_3(N - 1)

    with jax.named_scope("mine"):
        def mine(i, carry):
            out_ref[pl.ds(pl.multiple_of(i * AW, AW), AW), :] = dot(i, 1, 0, 4)
            return carry

        lax.fori_loop(0, 4, mine, 0)

    def z1_wait(m):
        for k, cells in parts(m):
            wait(precv.at[(0, *cells)], z1_r.at[m, k])

    with jax.named_scope("finish_early"):
        for m in range(4):
            for k, cells in parts(m):
                for h, rows in HALVES:
                    wait(precv.at[(1, *cells, rows)], ry_r.at[m, k, h])
        for m in range(3):
            wait(precv.at[2, m], z3_r.at[m])
            z1_wait(m)

        def early(t, carry):
            finish(lax.div(t, 3), lax.rem(t, 3))
            return carry

        lax.fori_loop(0, 9, early, 0)
    with jax.named_scope("finish_late"):
        wait(precv.at[2, 3], z3_r.at[3])
        for k, cells in parts(3):
            wait(precv.at[(0, *cells)], z1_r.at[3, k])

            def late(t, carry, k=k):
                finish(*((t, 3) if k else (3, t)))
                return carry

            lax.fori_loop(0, 4 - k, late, 0)

    lo_mine[...] = jnp.sum(lo_sum[...], 0, keepdims=True)
    xs, ys4, cs = (x, x1, x2, x3), (y, y1, y2, y3), (c, other)
    z4 = ((zl, zh), (1 - zl, zh), (zl, 1 - zh), (1 - zl, 1 - zh))
    steps = [(i, j, k, l) for i in range(4) for j in range(4) for k in range(4) for l in range(2)][1:]
    far_first = sorted(steps, key=lambda t: -((0, 1, 2, 1)[t[0]] + (0, 1, 2, 1)[t[1]] + (0, 1, 2, 1)[t[2]]))
    for r, (i, j, k, l) in enumerate(far_first):
        p = dev(x_=xs[i], y_=ys4[j], c_=cs[l], zl_=z4[k][0], zh_=z4[k][1])
        send(lo_mine, lo_in.at[r], lo_s, lo_r, p)
    with jax.named_scope("loss"):
        wait(lo_in, lo_r)
    loss_ref[...] = jnp.sum(lo_mine[...] + jnp.sum(lo_in[...], 0), axis=1, keepdims=True) / width

    with jax.named_scope("drain"):
        wait(a_ref.at[:, 0:6144], s1a_s)
        wait(b_ref.at[:, 0:7168], s1b_s)
        for n in range(N):
            for k in range(2):
                wait(av.at[n, x, :, c], aga_s.at[n, k])
                wait(bv.at[n, :, y], agb_s.at[n, k])
                wait(av.at[n, x, 0:2, c], rla_s.at[n, k])
                wait(bv.at[n, 0:2, y], rlb_s.at[n, k])
            for k in range(4):
                wait(av.at[n, x, :, c], dd_s.at[n, k])
        for m in range(4):
            for k, cells in parts(m):
                wait(precv.at[(0, *cells)], z1_s.at[m, k])
                for h, rows in HALVES:
                    wait(prelay.at[(h, *cells)], fr_s.at[m, k, h])
                    wait(prelay.at[(h, *cells)], ry_s.at[m, k, h])
            wait(precv.at[2, m], z3_s.at[m])
        wait(ma_in, mo_s.at[0])
        wait(mb_in, mo_s.at[1])
        wait(ma_zin, mo_s.at[2])
        wait(mb_zin, mo_s.at[3])
        wait(lo_in, lo_s)


def shards(view_a, view_b):
    rows, width = view_a.shape
    count = rows * 128
    dma = pltpu.SemaphoreType.DMA
    vm = pltpu.VMEM
    out, loss = pl.pallas_call(
        lambda *refs: kernel(float(count), float(width), *refs),
        out_shape=(pltpu.VMEM((1024, 512), F32), pltpu.VMEM((1, 1), F32)),
        in_specs=[pl.BlockSpec(memory_space=pl.ANY)] * 2,
        out_specs=(pl.BlockSpec(memory_space=pltpu.VMEM), pl.BlockSpec(memory_space=pltpu.VMEM)),
        scratch_shapes=[
            vm((S, width), BF16), vm((S, width), BF16), dma((2,)),
            vm((N, 4, 4, 2, S, AW), BF16),
            vm((N, 4, 4, 2, S, BW), BF16),
            vm((N, AW, K), BF16),
            vm((2, K, 4 * BW), BF16),
            vm((3, 4, 4, AW, BW), BF16),
            vm((3, 4, 4, AW, BW), BF16),
            vm((2, 4, 4, AW // 2, BW), BF16),
            vm((N, 2, AW), F32), vm((7, N, 2, AW), F32), vm((N, 2, AW), F32), vm((3, N, 2, AW), F32),
            vm((N, 2, BW), F32), vm((3, N, 2, BW), F32), vm((N, 2, BW), F32), vm((3, N, 2, BW), F32),
            vm((N, 2, AW), F32), vm((N, 2, BW), F32),
            vm((8, 128), F32), vm((1, 128), F32), vm((127, 1, 128), F32),
            dma, dma((N,)), dma, dma((N,)),
            dma((N, 2)), dma((N, 2)), dma((N, 2)), dma((N, 2)), dma((N, 4)), dma((N, 4)),
            dma((N, 2)), dma((N, 2)), dma((N, 2)), dma((N, 2)),
            dma((4, 2)), dma((4, 2)), dma((4,)), dma((4,)),
            dma((4, 2, 2)), dma((4, 2, 2)), dma((4, 2, 2)), dma((4, 2, 2)),
            dma((4,)), dma((4,)), dma, dma,
        ],
        compiler_params=pltpu.CompilerParams(
            collective_id=0, has_side_effects=True, vmem_limit_bytes=59_000_000),
    )(view_a, view_b)
    return out, loss.reshape(())


def solution(mesh):
    finer = Mesh(mesh.devices.reshape(2, 4, 4, 2, 2), ROW_COL)
    in_specs = (P(ROW_COL, None), P(ROW_COL, None))
    out_specs = (P(ROW, COL), P())
    return jax.shard_map(
        shards, mesh=finer, in_specs=in_specs, out_specs=out_specs, check_vma=False
    )
```

```python
import jax
import jax.numpy as jnp
from jax import lax
from jax.experimental import pallas as pl
from jax.experimental.pallas import tpu as pltpu
from jax.sharding import Mesh
from jax.sharding import PartitionSpec as P

ROW = ("row_0", "row_1")
COL = ("col_0", "col_1", "col_2")
ROW_COL = ("row_0", "row_1", "col_0", "col_1", "col_2")

MESH = pl.DeviceIdType.MESH
F32 = jnp.float32
BF16 = jnp.bfloat16

N = 8
S = 96
AW = 256
BW = 128
GS = 384
K = 3072


def encode(v):
    return (v * v * (v * jnp.abs(v))).astype(BF16)


def decode(v):
    v = v.astype(F32)
    root = jnp.sqrt(jnp.sqrt(jnp.abs(v)))
    return jnp.where(v < 0.0, -root, root)


def kernel(count, width, a_hbm, b_hbm, out_ref, loss_ref,
           a_ref, b_ref, in_s, av, bv, at, bn, psend, precv, prelay,
           ma_mine, ma_in, ma_sum, mb_mine, mb_in, mb_sum, sta, stb,
           lo_sum, lo_mine, lo_in,
           s1a_s, s1a_r, s1b_s, s1b_r, a_s, b_s, z_s, ma_s, mb_s, lo_s,
           aga_r, rla_r, dd_r, ddf_r, agb_r, rlb_r, z1_r, z3_r, fr_r, mo_r, lo_r):
    zl, y, x, zh, c = (lax.axis_index(n) for n in ROW_COL)

    def scoped(f):
        def g(q, *rest):
            with jax.named_scope(f"{f.__name__}_{q}"):
                return f(q, *rest)
        return g

    def dev(x_=None, y_=None, c_=None, zl_=None, zh_=None):
        return (zl if zl_ is None else zl_, y if y_ is None else y_, x if x_ is None else x_,
                zh if zh_ is None else zh_, c if c_ is None else c_)

    def ring(v, d):
        return lax.rem(v + d, 4)

    def xc(r):
        t = lax.rem(x * 2 + c + r, 8)
        return lax.div(t, 2), lax.rem(t, 2)

    def send(src, dst, ss, rs, device):
        pltpu.make_async_remote_copy(src_ref=src, dst_ref=dst, send_sem=ss, recv_sem=rs,
                                     device_id=device, device_id_type=MESH).start()

    def wait(ref, sem):
        pltpu.make_async_copy(ref, ref, sem).wait()

    x1, x2, x3 = ring(x, 1), ring(x, 2), ring(x, 3)
    y1, y2, y3 = ring(y, 1), ring(y, 2), ring(y, 3)
    other = 1 - c
    p1 = dev(zl_=1 - zl)
    p2 = dev(zh_=1 - zh)
    p3 = dev(zl_=1 - zl, zh_=1 - zh)
    xcs = [dev(x_=xc(r)[0], c_=xc(r)[1]) for r in range(1, 8)]
    ys = [dev(y_=v) for v in (y1, y2, y3)]
    zs = [p1, p2, p3]
    load_a = pltpu.make_async_copy(a_hbm, a_ref, in_s.at[0])
    load_b = pltpu.make_async_copy(b_hbm, b_ref, in_s.at[1])
    load_a.start()
    load_b.start()

    barrier = pltpu.get_barrier_semaphore()
    peers = xcs + ys + zs
    with jax.named_scope("barrier"):
        for p in peers:
            pl.semaphore_signal(barrier, inc=1, device_id=p, device_id_type=MESH)
        pl.semaphore_wait(barrier, len(peers))
    load_a.wait()
    load_b.wait()

    def stage1(n, carry):
        k = lax.rem(n, 4)
        ha = lax.rem(zl + lax.div(n, 4), 2)
        hb = lax.rem(zh + 1 + lax.div(n, 4), 2)
        for d in (1, 3, 2, 0):
            yp = ring(y, d)
            cols = pl.ds(pl.multiple_of(ha * 4096 + yp * 1024 + k * AW, AW), AW)
            dst = av.at[n, x, y, c]
            if d:
                send(a_ref.at[:, cols], dst, s1a_s, s1a_r.at[n], dev(y_=yp))
            else:
                pltpu.make_async_copy(a_hbm.at[:, cols], dst, s1a_r.at[n]).start()
        for r in (1, 2, 3, 7, 6, 5, 4, 0):
            px, pc = xc(r)
            cols = pl.ds(pl.multiple_of(px * 2048 + hb * 1024 + pc * 512 + k * BW, BW), BW)
            dst = bv.at[n, x, y, c]
            if r:
                send(b_ref.at[:, cols], dst, s1b_s, s1b_r.at[n], dev(x_=px, c_=pc))
            else:
                pltpu.make_async_copy(b_hbm.at[:, cols], dst, s1b_r.at[n]).start()
        return carry

    with jax.named_scope("stage1"):
        lax.fori_loop(0, N, stage1, 0)

    def s1_wait(n):
        wait(av.at[n, x, :, c], s1a_r.at[n])
        wait(bv.at[n, :, y], s1b_r.at[n])

    def own_part(n, up, down, k):
        for part, px, py in ((up, x1, y1), (down, x3, y3)):
            a = av.at[n, x, part, c]
            send(a, a, a_s, aga_r.at[k], dev(x_=px))
            b = bv.at[n, part, y]
            send(b, b, b_s, agb_r.at[k], dev(y_=py))

    ALL, LOW, HIGH = pl.ds(0, 4), pl.ds(0, 2), pl.ds(2, 2)

    @scoped
    def own(n):
        if n < N - 1:
            own_part(n, ALL, ALL, n)
        else:
            own_part(n, LOW, HIGH, n)
            own_part(n, HIGH, LOW, N)
        a = av.at[n, x, :, c]
        send(a, a, a_s, dd_r.at[n], dev(c_=other))

    def own_moments(n):
        def one(k, acc):
            sa, qa, sb, qb = acc
            va = av[n, x, lax.div(k, 2), c, pl.ds(pl.multiple_of(lax.rem(k, 2) * 48, 16), 48), :].astype(F32)
            va = va.reshape(6, 8, AW)
            sa = sa + jnp.sum(va, 0)
            qa = qa + jnp.sum(va * va, 0)
            vb = bv[n, lax.div(k, 2), y, lax.rem(k, 2)].astype(F32).reshape(12, 8, BW)
            sb = sb + jnp.sum(vb, 0)
            qb = qb + jnp.sum(vb * vb, 0)
            return sa, qa, sb, qb

        za, zb = jnp.zeros((8, AW), F32), jnp.zeros((8, BW), F32)
        sa, qa, sb, qb = lax.fori_loop(0, 8, one, (za, za, zb, zb))
        ma_mine[n, 0:1, :] = jnp.sum(sa, 0, keepdims=True)
        ma_mine[n, 1:2, :] = jnp.sum(qa, 0, keepdims=True)
        mb_mine[n, 0:1, :] = jnp.sum(sb, 0, keepdims=True)
        mb_mine[n, 1:2, :] = jnp.sum(qb, 0, keepdims=True)

    def relay(n):
        for v, part, px in ((x3, LOW, x1), (x1, HIGH, x3)):
            a = av.at[n, v, part, c]
            send(a, a, a_s, rla_r.at[n], dev(x_=px))
        for v, part, py in ((y3, LOW, y1), (y1, HIGH, y3)):
            b = bv.at[n, part, v]
            send(b, b, b_s, rlb_r.at[n], dev(y_=py))

    def share(n, part3, part1):
        for v, part in ((x3, part3), (x1, part1)):
            a = av.at[n, v, part, c]
            send(a, a, a_s, dd_r.at[n], dev(c_=other))

    @scoped
    def arrive(n):
        wait(av.at[n, 0:2, :, c], aga_r.at[n])
        wait(bv.at[n, :, 0:2], agb_r.at[n])
        relay(n)
        share(n, ALL, ALL)

    @scoped
    def arrive_first(n):
        wait(av.at[n, 0, :, c], aga_r.at[n])
        wait(bv.at[n, :, 0], agb_r.at[n])
        relay(n)
        share(n, LOW, HIGH)

    @scoped
    def arrive_second(n):
        wait(av.at[n, 0, :, c], aga_r.at[n + 1])
        wait(bv.at[n, :, 0], agb_r.at[n + 1])
        share(n, HIGH, LOW)

    def wait_and_sum(n, carry):
        s1_wait(n)
        own_moments(n)
        return carry

    with jax.named_scope("s1_wait"):
        s1_wait(0)
        own(0)
        own_moments(0)
        lax.fori_loop(1, N, wait_and_sum, 0)
    for r, p in enumerate(xcs):
        send(ma_mine, ma_in.at[r], ma_s, mo_r.at[0], p)
    for r, p in enumerate(ys):
        send(mb_mine, mb_in.at[r], mb_s, mo_r.at[1], p)
    own(1)
    arrive(0)
    own(2)
    with jax.named_scope("mom_1"):
        wait(ma_in.at[0:7], mo_r.at[0])
        wait(mb_in.at[0:3], mo_r.at[1])
    ma_sum[...] = ma_mine[...] + jnp.sum(ma_in[0:7], 0)
    mb_sum[...] = mb_mine[...] + jnp.sum(mb_in[0:3], 0)
    for r, p in enumerate(zs):
        send(ma_sum, ma_in.at[7 + r], ma_s, mo_r.at[2], p)
        send(mb_sum, mb_in.at[3 + r], mb_s, mo_r.at[3], p)
    arrive(1)
    own(3)

    def moments_done():
        with jax.named_scope("mom_2"):
            wait(ma_in.at[7:10], mo_r.at[2])
            wait(mb_in.at[3:6], mo_r.at[3])
        for mine, zin, z0, st, turn in ((ma_sum, ma_in, 7, sta, (4, 0, 4)), (mb_sum, mb_in, 3, stb, (0, 4, 4))):
            for n in range(N):
                total = (mine[n] + zin[z0, (n + turn[0]) % N] + zin[z0 + 1, (n + turn[1]) % N]
                         + zin[z0 + 2, (n + turn[2]) % N])
                mean = total[0:1, :] / count
                var = total[1:2, :] / count - mean * mean
                st[n, 0:1, :] = mean
                st[n, 1:2, :] = lax.rsqrt(var + 1e-05)

    @scoped
    def far(n):
        wait(av.at[n, x2, :, c], rla_r.at[n])
        a = av.at[n, x2, :, c]
        send(a, a, a_s, ddf_r.at[n], dev(c_=other))
        wait(bv.at[n, :, y2], rlb_r.at[n])

    def norm_a(n, lo, hi):
        def group(g, carry):
            x0, yh = ring(x2 + 1, lax.div(g, 2)), lax.rem(g, 2)
            at_ = pl.multiple_of((x0 * 2 + yh) * GS, 128)
            for m in range(AW // 128):
                cols = pl.ds(m * 128, 128)
                v = av[n, x0, pl.ds(yh * 2, 2), :, :, cols].reshape(GS, 128).astype(F32)
                v = ((v - sta[n, 0:1, cols]) * sta[n, 1:2, cols]).astype(BF16)
                at[n, cols, pl.ds(at_, GS)] = v.T
            return carry

        lax.fori_loop(lo, hi, group, 0)

    def norm_b(n, lo, hi):
        cols = pl.ds((n % 4) * BW, BW)

        def group(g, carry):
            x0, yh = lax.rem(g, 4), lax.rem(lax.div(y2, 2) + 1 + lax.div(g, 4), 2)
            at_ = pl.multiple_of((x0 * 2 + yh) * GS, 128)
            v = bv[n, x0, pl.ds(yh * 2, 2)].reshape(GS, BW).astype(F32)
            v = ((v - stb[n, 0:1, :]) * stb[n, 1:2, :]).astype(BF16)
            bn[n // 4, pl.ds(at_, GS), cols] = v
            return carry

        lax.fori_loop(lo, hi, group, 0)

    @scoped
    def near_norm(n):
        wait(av.at[n, 0:3, :, other], dd_r.at[n])
        norm_a(n, 0, 6)
        norm_b(n, 0, 4)

    @scoped
    def far_norm(n):
        wait(av.at[n, x2, :, other], ddf_r.at[n])
        norm_a(n, 6, 8)
        norm_b(n, 4, 8)

    def dot(i, half, j, n):
        r = jnp.dot(at[i], bn[half, :, j * BW:(j + n) * BW], preferred_element_type=F32)
        return r * (1.0 / count)

    def keep(slot, i, j, v):
        if slot == 1:
            psend[slot, i, j] = encode(v)
        elif slot == 0:
            psend[slot, i, j, 0:128] = encode(v[0:128])
            psend[slot, i, j, 128:256] = encode(v[128:256] + decode(prelay[1, i, j]))
        else:
            psend[slot, i, j, 0:128] = encode(v[0:128] + decode(prelay[0, i, j]))
            psend[slot, i, j, 128:256] = encode(v[128:256])

    def row(slot, m, i, half, n):
        r = dot(i, half, 0, n)
        for j in range(n):
            keep(slot, m, j, r[:, j * BW:(j + 1) * BW])

    def column(slot, m, base, half):
        def one(i, carry):
            keep(slot, i, m, dot(base + i, half, m, 1))
            return carry

        lax.fori_loop(0, m, one, 0)

    def far_wait(m, h):
        wait(bn.at[0, pl.ds(0, 32 * (2 * m + 1))], fr_r.at[m, h])

    def parts(m):
        yield 0, (m, pl.ds(0, m + 1))
        if m:
            yield 1, (pl.ds(0, m), m)

    HALVES = ((0, pl.ds(0, 128)), (1, pl.ds(128, 128)))

    @scoped
    def multiply_far(m):
        row(1, m, m, 0, m + 1)
        column(1, m, 0, 0)
        for k, cells in parts(m):
            for h, rows in HALVES:
                send(psend.at[(1, *cells, rows)], prelay.at[(h, *cells)],
                     z_s, fr_r.at[m, h], (p1, p3)[h])

    def send_1(m, k):
        for kk, cells in parts(m):
            if kk == k:
                send(psend.at[(0, *cells)], precv.at[(0, *cells)], z_s, z1_r.at[k + 1 if m == 3 else 0], p1)

    @scoped
    def row_1(n):
        far_wait(n - 4, 1)
        row(0, n - 4, n, 1, n - 3)
        send_1(n - 4, 0)

    @scoped
    def column_1(n):
        column(0, n - 4, 4, 1)
        send_1(n - 4, 1)

    @scoped
    def multiply_3(n):
        m = n - 4
        if m == 0:
            for k in range(4):
                far_wait(k, 0)
        row(2, m, n, 0, 4)
        send(psend.at[2, m], precv.at[1, m], z_s, z3_r.at[m // 3], p3)

    row0 = (zl * 4 + y) * 1024
    col0 = ((x * 2 + zh) * 2 + c) * 512

    def finish(i, j):
        at_ = (pl.ds(pl.multiple_of(i * AW, AW), AW), pl.ds(pl.multiple_of(j * BW, BW), BW))
        v = out_ref[at_] + (decode(precv[0, i, j]) + decode(precv[1, i, j]))
        out_ref[at_] = v
        rows = row0 + i * AW + lax.broadcasted_iota(jnp.int32, (AW, BW), 0)
        cols = col0 + j * BW + lax.broadcasted_iota(jnp.int32, (AW, BW), 1)
        term = jnp.where(rows == cols, (1.0 - v) * (1.0 - v), 0.0051 * (v * v))
        lo_sum[...] += jnp.sum(term.reshape(AW // 8, 8, BW), 0)

    lo_sum[...] = jnp.zeros_like(lo_sum)
    moments_done()
    for n in range(1, N - 1):
        if n > 1:
            arrive(n)
            if n + 2 < N - 1:
                own(n + 2)
            elif n + 1 == N - 1:
                own(N - 1)
        near_norm(n - 1)
        if n == N - 2:
            multiply_3(4)
        far(n - 1)
        far_norm(n - 1)
        if n < 5:
            multiply_far(n - 1)
        else:
            row_1(n - 1)
            column_1(n - 1)
    near_norm(N - 2)
    far(N - 2)
    arrive_first(N - 1)
    multiply_3(5)
    far_norm(N - 2)
    row_1(N - 2)
    arrive_second(N - 1)
    column_1(N - 2)
    near_norm(N - 1)
    far(N - 1)
    multiply_3(6)
    far_norm(N - 1)
    row_1(N - 1)
    column_1(N - 1)
    multiply_3(N - 1)

    with jax.named_scope("mine"):
        def mine(i, carry):
            out_ref[pl.ds(pl.multiple_of(i * AW, AW), AW), :] = dot(i, 1, 0, 4)
            return carry

        lax.fori_loop(0, 4, mine, 0)

    with jax.named_scope("finish_early"):
        wait(precv.at[1, 0:3], z3_r.at[0])
        wait(precv.at[0, 0:3, 0:3], z1_r.at[0])

        def early(t, carry):
            finish(lax.div(t, 3), lax.rem(t, 3))
            return carry

        lax.fori_loop(0, 9, early, 0)
    with jax.named_scope("finish_late"):
        wait(precv.at[1, 3], z3_r.at[1])
        for k, cells in parts(3):
            wait(precv.at[(0, *cells)], z1_r.at[k + 1])

            def late(t, carry, k=k):
                finish(*((t, 3) if k else (3, t)))
                return carry

            lax.fori_loop(0, 4 - k, late, 0)

    lo_mine[...] = jnp.sum(lo_sum[...], 0, keepdims=True)
    xs, ys4, cs = (x, x1, x2, x3), (y, y1, y2, y3), (c, other)
    z4 = ((zl, zh), (1 - zl, zh), (zl, 1 - zh), (1 - zl, 1 - zh))
    steps = [(i, j, k, l) for i in range(4) for j in range(4) for k in range(4) for l in range(2)][1:]
    far_first = sorted(steps, key=lambda t: -((0, 1, 2, 1)[t[0]] + (0, 1, 2, 1)[t[1]] + (0, 1, 2, 1)[t[2]]))
    for r, (i, j, k, l) in enumerate(far_first):
        p = dev(x_=xs[i], y_=ys4[j], c_=cs[l], zl_=z4[k][0], zh_=z4[k][1])
        send(lo_mine, lo_in.at[r], lo_s, lo_r, p)
    with jax.named_scope("loss"):
        wait(lo_in, lo_r)
    loss_ref[...] = jnp.sum(lo_mine[...] + jnp.sum(lo_in[...], 0), axis=1, keepdims=True) / width

    with jax.named_scope("drain"):
        wait(a_ref.at[:, 0:6144], s1a_s)
        wait(b_ref.at[:, 0:7168], s1b_s)
        wait(av.at[0:7], a_s)
        wait(bv.at[0:6], b_s)
        wait(psend, z_s)
        wait(ma_in, ma_s)
        wait(mb_in, mb_s)
        wait(lo_in, lo_s)


def shards(view_a, view_b):
    rows, width = view_a.shape
    count = rows * 128
    dma = pltpu.SemaphoreType.DMA
    vm = pltpu.VMEM
    out, loss = pl.pallas_call(
        lambda *refs: kernel(float(count), float(width), *refs),
        out_shape=(pltpu.VMEM((1024, 512), F32), pltpu.VMEM((1, 1), F32)),
        in_specs=[pl.BlockSpec(memory_space=pl.ANY)] * 2,
        out_specs=(pl.BlockSpec(memory_space=pltpu.VMEM), pl.BlockSpec(memory_space=pltpu.VMEM)),
        scratch_shapes=[
            vm((S, width), BF16), vm((S, width), BF16), dma((2,)),
            vm((N, 4, 4, 2, S, AW), BF16),
            vm((N, 4, 4, 2, S, BW), BF16),
            vm((N, AW, K), BF16),
            vm((2, K, 4 * BW), BF16),
            vm((3, 4, 4, AW, BW), BF16),
            vm((2, 4, 4, AW, BW), BF16),
            vm((2, 4, 4, AW // 2, BW), BF16),
            vm((N, 2, AW), F32), vm((10, N, 2, AW), F32), vm((N, 2, AW), F32),
            vm((N, 2, BW), F32), vm((6, N, 2, BW), F32), vm((N, 2, BW), F32),
            vm((N, 2, AW), F32), vm((N, 2, BW), F32),
            vm((8, 128), F32), vm((1, 128), F32), vm((127, 1, 128), F32),
            dma, dma((N,)), dma, dma((N,)), dma, dma, dma, dma, dma, dma,
            dma((N + 1,)), dma((N,)), dma((N,)), dma((N,)), dma((N + 1,)), dma((N,)),
            dma((3,)), dma((2,)), dma((4, 2)), dma((4,)), dma,
        ],
        compiler_params=pltpu.CompilerParams(
            collective_id=0, has_side_effects=True, vmem_limit_bytes=59_000_000),
    )(view_a, view_b)
    return out, loss.reshape(())


def solution(mesh):
    finer = Mesh(mesh.devices.reshape(2, 4, 4, 2, 2), ROW_COL)
    in_specs = (P(ROW_COL, None), P(ROW_COL, None))
    out_specs = (P(ROW, COL), P())
    return jax.shard_map(
        shards, mesh=finer, in_specs=in_specs, out_specs=out_specs, check_vma=False
    )
```

```python
import jax
import jax.numpy as jnp
from jax import lax
from jax.experimental import pallas as pl
from jax.experimental.pallas import tpu as pltpu
from jax.sharding import Mesh
from jax.sharding import PartitionSpec as P

ROW = ("row_0", "row_1")
COL = ("col_0", "col_1", "col_2")
ROW_COL = ("row_0", "row_1", "col_0", "col_1", "col_2")

MESH = pl.DeviceIdType.MESH
F32 = jnp.float32
BF16 = jnp.bfloat16

N = 8
S = 96
AW = 256
BW = 128
GS = 384
K = 3072


def encode(v):
    return (v * v * (v * jnp.abs(v))).astype(BF16)


def decode(v):
    v = v.astype(F32)
    root = jnp.sqrt(jnp.sqrt(jnp.abs(v)))
    return jnp.where(v < 0.0, -root, root)


def kernel(count, width, a_hbm, b_hbm, out_ref, loss_ref,
           a_ref, b_ref, in_s, av, bv, at, bn, psend, precv, prelay,
           ma_mine, ma_in, ma_sum, ma_all, mb_mine, mb_in, mb_sum, sta, stb,
           held, lo_sum, lo_mine, lo_in,
           s1a_s, s1a_r, s1b_s, s1b_r, a_s, b_s, z_s, ma_s, mb_s, lo_s,
           aga_r, rla_r, dd_r, ddf_r, agb_r, rlb_r, z1_r, z3_r, fr_r, mo_r, lo_r):
    zl, y, x, zh, c = (lax.axis_index(n) for n in ROW_COL)

    def scoped(f):
        def g(q, *rest):
            with jax.named_scope(f"{f.__name__}_{q}"):
                return f(q, *rest)
        return g

    def dev(x_=None, y_=None, c_=None, zl_=None, zh_=None):
        return (zl if zl_ is None else zl_, y if y_ is None else y_, x if x_ is None else x_,
                zh if zh_ is None else zh_, c if c_ is None else c_)

    def ring(v, d):
        return lax.rem(v + d, 4)

    def xc(r):
        t = lax.rem(x * 2 + c + r, 8)
        return lax.div(t, 2), lax.rem(t, 2)

    def send(src, dst, ss, rs, device):
        pltpu.make_async_remote_copy(src_ref=src, dst_ref=dst, send_sem=ss, recv_sem=rs,
                                     device_id=device, device_id_type=MESH).start()

    def wait(ref, sem):
        pltpu.make_async_copy(ref, ref, sem).wait()

    x1, x2, x3 = ring(x, 1), ring(x, 2), ring(x, 3)
    y1, y2, y3 = ring(y, 1), ring(y, 2), ring(y, 3)
    other = 1 - c
    p1 = dev(zl_=1 - zl)
    p2 = dev(zh_=1 - zh)
    p3 = dev(zl_=1 - zl, zh_=1 - zh)
    xcs = [dev(x_=xc(r)[0], c_=xc(r)[1]) for r in range(1, 8)]
    ys = [dev(y_=v) for v in (y1, y2, y3)]
    zs = [p1, p2, p3]
    load_a = pltpu.make_async_copy(a_hbm, a_ref, in_s.at[0])
    load_b = pltpu.make_async_copy(b_hbm, b_ref, in_s.at[1])
    load_a.start()
    load_b.start()

    barrier = pltpu.get_barrier_semaphore()
    peers = xcs + ys + zs
    with jax.named_scope("barrier"):
        for p in peers:
            pl.semaphore_signal(barrier, inc=1, device_id=p, device_id_type=MESH)
        pl.semaphore_wait(barrier, len(peers))
    load_a.wait()
    load_b.wait()

    def stage1(n, carry):
        k = lax.rem(n, 4)
        ha = lax.rem(zl + lax.div(n, 4), 2)
        hb = lax.rem(zh + 1 + lax.div(n, 4), 2)
        for d in (1, 3, 2, 0):
            yp = ring(y, d)
            cols = pl.ds(pl.multiple_of(ha * 4096 + yp * 1024 + k * AW, AW), AW)
            dst = av.at[n, x, y, c]
            if d:
                send(a_ref.at[:, cols], dst, s1a_s, s1a_r.at[n], dev(y_=yp))
            else:
                pltpu.make_async_copy(a_hbm.at[:, cols], dst, s1a_r.at[n]).start()
        for r in (1, 2, 3, 7, 6, 5, 4, 0):
            px, pc = xc(r)
            cols = pl.ds(pl.multiple_of(px * 2048 + hb * 1024 + pc * 512 + k * BW, BW), BW)
            dst = bv.at[n, x, y, c]
            if r:
                send(b_ref.at[:, cols], dst, s1b_s, s1b_r.at[n], dev(x_=px, c_=pc))
            else:
                pltpu.make_async_copy(b_hbm.at[:, cols], dst, s1b_r.at[n]).start()
        return carry

    with jax.named_scope("stage1"):
        lax.fori_loop(0, N, stage1, 0)

    def s1_wait(n):
        wait(av.at[n, x, :, c], s1a_r.at[n])
        wait(bv.at[n, :, y], s1b_r.at[n])

    def own_part(n, up, down, k):
        for part, px, py in ((up, x1, y1), (down, x3, y3)):
            a = av.at[n, x, part, c]
            send(a, a, a_s, aga_r.at[k], dev(x_=px))
            b = bv.at[n, part, y]
            send(b, b, b_s, agb_r.at[k], dev(y_=py))

    ALL, LOW, HIGH = pl.ds(0, 4), pl.ds(0, 2), pl.ds(2, 2)

    @scoped
    def own(n):
        if n < N - 1:
            own_part(n, ALL, ALL, n)
        else:
            own_part(n, LOW, HIGH, n)
            own_part(n, HIGH, LOW, N)
        a = av.at[n, x, :, c]
        send(a, a, a_s, dd_r.at[n], dev(c_=other))

    def own_moments(n):
        def one(k, acc):
            sa, qa, sb, qb = acc
            va = av[n, x, lax.div(k, 2), c, pl.ds(pl.multiple_of(lax.rem(k, 2) * 48, 16), 48), :].astype(F32)
            va = va.reshape(6, 8, AW)
            sa = sa + jnp.sum(va, 0)
            qa = qa + jnp.sum(va * va, 0)
            vb = bv[n, lax.div(k, 2), y, lax.rem(k, 2)].astype(F32).reshape(12, 8, BW)
            sb = sb + jnp.sum(vb, 0)
            qb = qb + jnp.sum(vb * vb, 0)
            return sa, qa, sb, qb

        za, zb = jnp.zeros((8, AW), F32), jnp.zeros((8, BW), F32)
        sa, qa, sb, qb = lax.fori_loop(0, 8, one, (za, za, zb, zb))
        ma_mine[n, 0:1, :] = jnp.sum(sa, 0, keepdims=True)
        ma_mine[n, 1:2, :] = jnp.sum(qa, 0, keepdims=True)
        mb_mine[n, 0:1, :] = jnp.sum(sb, 0, keepdims=True)
        mb_mine[n, 1:2, :] = jnp.sum(qb, 0, keepdims=True)

    def relay(n):
        for v, part, px in ((x3, LOW, x1), (x1, HIGH, x3)):
            a = av.at[n, v, part, c]
            send(a, a, a_s, rla_r.at[n], dev(x_=px))
        for v, part, py in ((y3, LOW, y1), (y1, HIGH, y3)):
            b = bv.at[n, part, v]
            send(b, b, b_s, rlb_r.at[n], dev(y_=py))

    def share(n, part3, part1):
        for v, part in ((x3, part3), (x1, part1)):
            a = av.at[n, v, part, c]
            send(a, a, a_s, dd_r.at[n], dev(c_=other))

    @scoped
    def arrive(n):
        wait(av.at[n, 0:2, :, c], aga_r.at[n])
        wait(bv.at[n, :, 0:2], agb_r.at[n])
        relay(n)
        share(n, ALL, ALL)

    @scoped
    def arrive_first(n):
        wait(av.at[n, 0, :, c], aga_r.at[n])
        wait(bv.at[n, :, 0], agb_r.at[n])
        relay(n)
        share(n, LOW, HIGH)

    @scoped
    def arrive_second(n):
        wait(av.at[n, 0, :, c], aga_r.at[n + 1])
        wait(bv.at[n, :, 0], agb_r.at[n + 1])
        share(n, HIGH, LOW)

    def wait_and_sum(n, carry):
        s1_wait(n)
        own_moments(n)
        return carry

    with jax.named_scope("s1_wait"):
        s1_wait(0)
        own(0)
        own_moments(0)
        lax.fori_loop(1, N, wait_and_sum, 0)
    send(ma_mine, ma_in.at[6], ma_s, mo_r.at[4], dev(c_=other))
    with jax.named_scope("mom_0"):
        wait(ma_in.at[6], mo_r.at[4])
    ma_sum[...] = ma_mine[...] + ma_in[6]
    for r, v in enumerate((x1, x2, x3)):
        send(ma_sum, ma_in.at[r], ma_s, mo_r.at[0], dev(x_=v))
    for r, p in enumerate(ys):
        send(mb_mine, mb_in.at[r], mb_s, mo_r.at[1], p)
    own(1)
    arrive(0)
    own(2)
    with jax.named_scope("mom_1"):
        wait(ma_in.at[0:3], mo_r.at[0])
        wait(mb_in.at[0:3], mo_r.at[1])
    ma_all[...] = ma_sum[...] + jnp.sum(ma_in[0:3], 0)
    mb_sum[...] = mb_mine[...] + jnp.sum(mb_in[0:3], 0)
    for r, p in enumerate(zs):
        send(ma_all, ma_in.at[3 + r], ma_s, mo_r.at[2], p)
        send(mb_sum, mb_in.at[3 + r], mb_s, mo_r.at[3], p)
    arrive(1)
    own(3)

    def moments_done():
        with jax.named_scope("mom_2"):
            wait(ma_in.at[3:6], mo_r.at[2])
            wait(mb_in.at[3:6], mo_r.at[3])
        for mine, zin, z0, st, turn in ((ma_all, ma_in, 3, sta, (4, 0, 4)), (mb_sum, mb_in, 3, stb, (0, 4, 4))):
            for n in range(N):
                total = (mine[n] + zin[z0, (n + turn[0]) % N] + zin[z0 + 1, (n + turn[1]) % N]
                         + zin[z0 + 2, (n + turn[2]) % N])
                mean = total[0:1, :] / count
                var = total[1:2, :] / count - mean * mean
                st[n, 0:1, :] = mean
                st[n, 1:2, :] = lax.rsqrt(var + 1e-05)

    @scoped
    def far(n):
        wait(av.at[n, x2, :, c], rla_r.at[n])
        a = av.at[n, x2, :, c]
        send(a, a, a_s, ddf_r.at[n], dev(c_=other))
        wait(bv.at[n, :, y2], rlb_r.at[n])

    def norm_a(n, lo, hi):
        def group(g, carry):
            x0, yh = ring(x2 + 1, lax.div(g, 2)), lax.rem(g, 2)
            at_ = pl.multiple_of((x0 * 2 + yh) * GS, 128)
            for m in range(AW // 128):
                cols = pl.ds(m * 128, 128)
                v = av[n, x0, pl.ds(yh * 2, 2), :, :, cols].reshape(GS, 128).astype(F32)
                v = ((v - sta[n, 0:1, cols]) * sta[n, 1:2, cols]).astype(BF16)
                at[n, cols, pl.ds(at_, GS)] = v.T
            return carry

        lax.fori_loop(lo, hi, group, 0)

    def norm_b(n, lo, hi):
        cols = pl.ds((n % 4) * BW, BW)

        def group(g, carry):
            x0, yh = lax.rem(g, 4), lax.rem(lax.div(y2, 2) + 1 + lax.div(g, 4), 2)
            at_ = pl.multiple_of((x0 * 2 + yh) * GS, 128)
            v = bv[n, x0, pl.ds(yh * 2, 2)].reshape(GS, BW).astype(F32)
            v = ((v - stb[n, 0:1, :]) * stb[n, 1:2, :]).astype(BF16)
            bn[n // 4, pl.ds(at_, GS), cols] = v
            return carry

        lax.fori_loop(lo, hi, group, 0)

    @scoped
    def near_norm(n):
        wait(av.at[n, 0:3, :, other], dd_r.at[n])
        norm_a(n, 0, 6)
        norm_b(n, 0, 4)

    @scoped
    def far_norm(n):
        wait(av.at[n, x2, :, other], ddf_r.at[n])
        norm_a(n, 6, 8)
        norm_b(n, 4, 8)

    def dot(i, half, j, n):
        r = jnp.dot(at[i], bn[half, :, j * BW:(j + n) * BW], preferred_element_type=F32)
        return r * (1.0 / count)

    def keep(slot, i, j, v):
        if slot == 1:
            psend[slot, i, j] = encode(v)
        elif slot == 0:
            psend[slot, i, j, 0:128] = encode(v[0:128])
            psend[slot, i, j, 128:256] = encode(v[128:256] + decode(prelay[1, i, j]))
        else:
            psend[slot, i, j, 0:128] = encode(v[0:128] + decode(prelay[0, i, j]))
            psend[slot, i, j, 128:256] = encode(v[128:256])

    def row(slot, m, i, half, n):
        r = dot(i, half, 0, n)
        for j in range(n):
            keep(slot, m, j, r[:, j * BW:(j + 1) * BW])

    def column(slot, m, base, half):
        def one(i, carry):
            keep(slot, i, m, dot(base + i, half, m, 1))
            return carry

        lax.fori_loop(0, m, one, 0)

    def far_wait(m, h):
        wait(bn.at[0, pl.ds(0, 32 * (2 * m + 1))], fr_r.at[m, h])

    def parts(m):
        yield 0, (m, pl.ds(0, m + 1))
        if m:
            yield 1, (pl.ds(0, m), m)

    HALVES = ((0, pl.ds(0, 128)), (1, pl.ds(128, 128)))

    @scoped
    def multiply_far(m):
        for k, cells in parts(m):
            if k:
                column(1, m, 0, 0)
            else:
                row(1, m, m, 0, m + 1)
            for h, rows in HALVES:
                send(psend.at[(1, *cells, rows)], prelay.at[(h, *cells)],
                     z_s, fr_r.at[m, h], (p1, p3)[h])

    def send_1(cells, k):
        send(psend.at[(0, *cells)], precv.at[(0, *cells)], z_s, z1_r.at[k], p1)

    @scoped
    def row_1(n):
        m = n - 4
        far_wait(m, 1)
        r = dot(n, 1, 0, m + 1)
        for j in range(m + 1):
            keep(0, m, j, r[:, j * BW:(j + 1) * BW])
            if m == 3:
                send_1((m, j), 1 + j)
        if m < 3:
            send_1((m, pl.ds(0, m + 1)), 0)

    @scoped
    def column_1(n):
        m = n - 4

        def one(i, carry):
            keep(0, i, m, dot(4 + i, 1, m, 1))
            if m == 3:
                send_1((i, m), 5 + i)
            return carry

        lax.fori_loop(0, m, one, 0)
        if 0 < m < 3:
            send_1((pl.ds(0, m), m), 0)

    @scoped
    def multiply_3(n):
        m = n - 4
        if m == 0:
            for k in range(4):
                far_wait(k, 0)
            r = held[...]
        else:
            r = dot(n, 0, 0, 4)
        for j in range(4):
            keep(2, m, j, r[:, j * BW:(j + 1) * BW])
            if m == 3:
                send(psend.at[2, m, j], precv.at[1, m, j], z_s, z3_r.at[1 + j], p3)
        if m < 3:
            send(psend.at[2, m], precv.at[1, m], z_s, z3_r.at[0], p3)

    row0 = (zl * 4 + y) * 1024
    col0 = ((x * 2 + zh) * 2 + c) * 512

    def spot(i, j):
        return pl.ds(pl.multiple_of(i * AW, AW), AW), pl.ds(pl.multiple_of(j * BW, BW), BW)

    def add(slot, i, j):
        out_ref[spot(i, j)] = out_ref[spot(i, j)] + decode(precv[slot, i, j])

    def finish(slot, i, j):
        at_ = spot(i, j)
        v = out_ref[at_] + decode(precv[slot, i, j])
        out_ref[at_] = v
        rows = row0 + i * AW + lax.broadcasted_iota(jnp.int32, (AW, BW), 0)
        cols = col0 + j * BW + lax.broadcasted_iota(jnp.int32, (AW, BW), 1)
        term = jnp.where(rows == cols, (1.0 - v) * (1.0 - v), 0.0051 * (v * v))
        lo_sum[...] += jnp.sum(term.reshape(AW // 8, 8, BW), 0)

    lo_sum[...] = jnp.zeros_like(lo_sum)
    moments_done()
    for n in range(1, N - 1):
        if n > 1:
            arrive(n)
            if n + 2 < N - 1:
                own(n + 2)
            elif n + 1 == N - 1:
                own(N - 1)
        near_norm(n - 1)
        far(n - 1)
        if n == N - 2:
            multiply_3(4)
            near_norm(6)
        far_norm(n - 1)
        if n < 5:
            multiply_far(n - 1)
        if n == 5:
            row_1(4)
            held[...] = dot(4, 0, 0, 4)
    row_1(5)
    far(6)
    column_1(5)
    multiply_3(5)
    arrive_first(7)
    far_norm(6)
    row_1(6)
    arrive_second(7)
    column_1(6)
    multiply_3(6)
    far(7)
    near_norm(7)
    far_norm(7)
    row_1(7)
    column_1(7)
    multiply_3(7)

    with jax.named_scope("mine"):
        def mine(i, carry):
            out_ref[pl.ds(pl.multiple_of(i * AW, AW), AW), :] = dot(i, 1, 0, 4)
            return carry

        lax.fori_loop(0, 4, mine, 0)

    with jax.named_scope("finish_early"):
        wait(precv.at[1, 0:3], z3_r.at[0])

        def adds(t, carry):
            add(1, lax.div(t, 4), lax.rem(t, 4))
            return carry

        lax.fori_loop(0, 12, adds, 0)
        wait(precv.at[0, 0:3, 0:3], z1_r.at[0])

        def early(t, carry):
            finish(0, lax.div(t, 3), lax.rem(t, 3))
            return carry

        lax.fori_loop(0, 9, early, 0)
    with jax.named_scope("finish_late"):
        def late_row(t, carry):
            wait(precv.at[0, 3, t], z1_r.at[1 + t])
            add(0, 3, t)
            return carry

        def late_3(t, carry):
            wait(precv.at[1, 3, t], z3_r.at[1 + t])
            finish(1, 3, t)
            return carry

        def late_column(t, carry):
            wait(precv.at[0, t, 3], z1_r.at[5 + t])
            finish(0, t, 3)
            return carry

        lax.fori_loop(0, 4, late_row, 0)
        with jax.named_scope("late_3"):
            lax.fori_loop(0, 4, late_3, 0)
        with jax.named_scope("late_1"):
            lax.fori_loop(0, 3, late_column, 0)

    lo_mine[...] = jnp.sum(lo_sum[...], 0, keepdims=True)
    xs, ys4, cs = (x, x1, x2, x3), (y, y1, y2, y3), (c, other)
    z4 = ((zl, zh), (1 - zl, zh), (zl, 1 - zh), (1 - zl, 1 - zh))
    steps = [(i, j, k, l) for i in range(4) for j in range(4) for k in range(4) for l in range(2)][1:]
    far_first = sorted(steps, key=lambda t: -((0, 1, 2, 1)[t[0]] + (0, 1, 2, 1)[t[1]] + (0, 1, 2, 1)[t[2]]))
    for r, (i, j, k, l) in enumerate(far_first):
        p = dev(x_=xs[i], y_=ys4[j], c_=cs[l], zl_=z4[k][0], zh_=z4[k][1])
        send(lo_mine, lo_in.at[r], lo_s, lo_r, p)
    with jax.named_scope("loss"):
        wait(lo_in, lo_r)
    loss_ref[...] = jnp.sum(lo_mine[...] + jnp.sum(lo_in[...], 0), axis=1, keepdims=True) / width

    with jax.named_scope("drain"):
        wait(a_ref.at[:, 0:6144], s1a_s)
        wait(b_ref.at[:, 0:7168], s1b_s)
        wait(av.at[0:7], a_s)
        wait(bv.at[0:6], b_s)
        wait(psend, z_s)
        wait(ma_in, ma_s)
        wait(mb_in, mb_s)
        wait(lo_in, lo_s)


def shards(view_a, view_b):
    rows, width = view_a.shape
    count = rows * 128
    dma = pltpu.SemaphoreType.DMA
    vm = pltpu.VMEM
    out, loss = pl.pallas_call(
        lambda *refs: kernel(float(count), float(width), *refs),
        out_shape=(pltpu.VMEM((1024, 512), F32), pltpu.VMEM((1, 1), F32)),
        in_specs=[pl.BlockSpec(memory_space=pl.ANY)] * 2,
        out_specs=(pl.BlockSpec(memory_space=pltpu.VMEM), pl.BlockSpec(memory_space=pltpu.VMEM)),
        scratch_shapes=[
            vm((S, width), BF16), vm((S, width), BF16), dma((2,)),
            vm((N, 4, 4, 2, S, AW), BF16),
            vm((N, 4, 4, 2, S, BW), BF16),
            vm((N, AW, K), BF16),
            vm((2, K, 4 * BW), BF16),
            vm((3, 4, 4, AW, BW), BF16),
            vm((2, 4, 4, AW, BW), BF16),
            vm((2, 4, 4, AW // 2, BW), BF16),
            vm((N, 2, AW), F32), vm((7, N, 2, AW), F32), vm((N, 2, AW), F32), vm((N, 2, AW), F32),
            vm((N, 2, BW), F32), vm((6, N, 2, BW), F32), vm((N, 2, BW), F32),
            vm((N, 2, AW), F32), vm((N, 2, BW), F32),
            vm((AW, 4 * BW), F32),
            vm((8, 128), F32), vm((1, 128), F32), vm((127, 1, 128), F32),
            dma, dma((N,)), dma, dma((N,)), dma, dma, dma, dma, dma, dma,
            dma((N + 1,)), dma((N,)), dma((N,)), dma((N,)), dma((N + 1,)), dma((N,)),
            dma((8,)), dma((5,)), dma((4, 2)), dma((5,)), dma,
        ],
        compiler_params=pltpu.CompilerParams(
            collective_id=0, has_side_effects=True, vmem_limit_bytes=59_000_000),
    )(view_a, view_b)
    return out, loss.reshape(())


def solution(mesh):
    finer = Mesh(mesh.devices.reshape(2, 4, 4, 2, 2), ROW_COL)
    in_specs = (P(ROW_COL, None), P(ROW_COL, None))
    out_specs = (P(ROW, COL), P())
    return jax.shard_map(
        shards, mesh=finer, in_specs=in_specs, out_specs=out_specs, check_vma=False
    )
```

```python
import jax
import jax.numpy as jnp
from jax import lax
from jax.experimental import pallas as pl
from jax.experimental.pallas import tpu as pltpu
from jax.sharding import Mesh
from jax.sharding import PartitionSpec as P

ROW = ("row_0", "row_1")
COL = ("col_0", "col_1", "col_2")
ROW_COL = ("row_0", "row_1", "col_0", "col_1", "col_2")

MESH = pl.DeviceIdType.MESH
F32 = jnp.float32
BF16 = jnp.bfloat16

N = 8
S = 96
AW = 256
BW = 128
GS = 384
K = 3072


def encode(v):
    return (v * v * (v * jnp.abs(v))).astype(BF16)


def decode(v):
    v = v.astype(F32)
    root = jnp.sqrt(jnp.sqrt(jnp.abs(v)))
    return jnp.where(v < 0.0, -root, root)


def kernel(count, width, a_hbm, b_hbm, out_ref, loss_ref,
           a_ref, b_ref, in_s, av, bv, at, bn, psend, precv, prelay,
           ma_mine, ma_in, ma_sum, ma_all, mb_mine, mb_in, mb_sum, sta, stb,
           held, lo_sum, lo_mine, lo_in,
           s1a_s, s1a_r, s1b_s, s1b_r, a_s, b_s, z_s, ma_s, mb_s, lo_s,
           aga_r, rla_r, dd_r, ddf_r, agb_r, rlb_r, z1_r, z3_r, fr_r, mo_r, lo_r):
    zl, y, x, zh, c = (lax.axis_index(n) for n in ROW_COL)

    def scoped(f):
        def g(q, *rest):
            with jax.named_scope(f"{f.__name__}_{q}"):
                return f(q, *rest)
        return g

    def dev(x_=None, y_=None, c_=None, zl_=None, zh_=None):
        return (zl if zl_ is None else zl_, y if y_ is None else y_, x if x_ is None else x_,
                zh if zh_ is None else zh_, c if c_ is None else c_)

    def ring(v, d):
        return lax.rem(v + d, 4)

    def xc(r):
        t = lax.rem(x * 2 + c + r, 8)
        return lax.div(t, 2), lax.rem(t, 2)

    def send(src, dst, ss, rs, device):
        pltpu.make_async_remote_copy(src_ref=src, dst_ref=dst, send_sem=ss, recv_sem=rs,
                                     device_id=device, device_id_type=MESH).start()

    def wait(ref, sem):
        pltpu.make_async_copy(ref, ref, sem).wait()

    x1, x2, x3 = ring(x, 1), ring(x, 2), ring(x, 3)
    y1, y2, y3 = ring(y, 1), ring(y, 2), ring(y, 3)
    other = 1 - c
    p1 = dev(zl_=1 - zl)
    p2 = dev(zh_=1 - zh)
    p3 = dev(zl_=1 - zl, zh_=1 - zh)
    xcs = [dev(x_=xc(r)[0], c_=xc(r)[1]) for r in range(1, 8)]
    ys = [dev(y_=v) for v in (y1, y2, y3)]
    zs = [p1, p2, p3]
    load_a = pltpu.make_async_copy(a_hbm, a_ref, in_s.at[0])
    load_b = pltpu.make_async_copy(b_hbm, b_ref, in_s.at[1])
    load_a.start()
    load_b.start()

    barrier = pltpu.get_barrier_semaphore()
    peers = xcs + ys + zs
    with jax.named_scope("barrier"):
        for p in peers:
            pl.semaphore_signal(barrier, inc=1, device_id=p, device_id_type=MESH)
        pl.semaphore_wait(barrier, len(peers))
    load_a.wait()
    load_b.wait()

    def stage1(n, carry):
        k = lax.rem(n, 4)
        ha = lax.rem(zl + lax.div(n, 4), 2)
        hb = lax.rem(zh + 1 + lax.div(n, 4), 2)
        for d in (1, 3, 2, 0):
            yp = ring(y, d)
            cols = pl.ds(pl.multiple_of(ha * 4096 + yp * 1024 + k * AW, AW), AW)
            dst = av.at[n, x, y, c]
            if d:
                send(a_ref.at[:, cols], dst, s1a_s, s1a_r.at[n], dev(y_=yp))
            else:
                pltpu.make_async_copy(a_hbm.at[:, cols], dst, s1a_r.at[n]).start()
        for r in (1, 2, 3, 7, 6, 5, 4, 0):
            px, pc = xc(r)
            cols = pl.ds(pl.multiple_of(px * 2048 + hb * 1024 + pc * 512 + k * BW, BW), BW)
            dst = bv.at[n, x, y, c]
            if r:
                send(b_ref.at[:, cols], dst, s1b_s, s1b_r.at[n], dev(x_=px, c_=pc))
            else:
                pltpu.make_async_copy(b_hbm.at[:, cols], dst, s1b_r.at[n]).start()
        return carry

    with jax.named_scope("stage1"):
        lax.fori_loop(0, N, stage1, 0)

    def s1_wait(n):
        wait(av.at[n, x, :, c], s1a_r.at[n])
        wait(bv.at[n, :, y], s1b_r.at[n])

    def own_part(n, up, down, k):
        for part, px, py in ((up, x1, y1), (down, x3, y3)):
            a = av.at[n, x, part, c]
            send(a, a, a_s, aga_r.at[k], dev(x_=px))
            b = bv.at[n, part, y]
            send(b, b, b_s, agb_r.at[k], dev(y_=py))

    ALL, LOW, HIGH = pl.ds(0, 4), pl.ds(0, 2), pl.ds(2, 2)

    @scoped
    def own(n):
        if n < N - 1:
            own_part(n, ALL, ALL, n)
        else:
            own_part(n, LOW, HIGH, n)
            own_part(n, HIGH, LOW, N)
        a = av.at[n, x, :, c]
        send(a, a, a_s, dd_r.at[n], dev(c_=other))

    def own_moments(n):
        def one(k, acc):
            sa, qa, sb, qb = acc
            va = av[n, x, lax.div(k, 2), c, pl.ds(pl.multiple_of(lax.rem(k, 2) * 48, 16), 48), :].astype(F32)
            va = va.reshape(6, 8, AW)
            sa = sa + jnp.sum(va, 0)
            qa = qa + jnp.sum(va * va, 0)
            vb = bv[n, lax.div(k, 2), y, lax.rem(k, 2)].astype(F32).reshape(12, 8, BW)
            sb = sb + jnp.sum(vb, 0)
            qb = qb + jnp.sum(vb * vb, 0)
            return sa, qa, sb, qb

        za, zb = jnp.zeros((8, AW), F32), jnp.zeros((8, BW), F32)
        sa, qa, sb, qb = lax.fori_loop(0, 8, one, (za, za, zb, zb))
        ma_mine[n, 0:1, :] = jnp.sum(sa, 0, keepdims=True)
        ma_mine[n, 1:2, :] = jnp.sum(qa, 0, keepdims=True)
        mb_mine[n, 0:1, :] = jnp.sum(sb, 0, keepdims=True)
        mb_mine[n, 1:2, :] = jnp.sum(qb, 0, keepdims=True)

    def relay(n):
        for v, part, px in ((x3, LOW, x1), (x1, HIGH, x3)):
            a = av.at[n, v, part, c]
            send(a, a, a_s, rla_r.at[n], dev(x_=px))
        for v, part, py in ((y3, LOW, y1), (y1, HIGH, y3)):
            b = bv.at[n, part, v]
            send(b, b, b_s, rlb_r.at[n], dev(y_=py))

    def share(n, part3, part1):
        for v, part in ((x3, part3), (x1, part1)):
            a = av.at[n, v, part, c]
            send(a, a, a_s, dd_r.at[n], dev(c_=other))

    @scoped
    def arrive(n):
        wait(av.at[n, 0:2, :, c], aga_r.at[n])
        wait(bv.at[n, :, 0:2], agb_r.at[n])
        relay(n)
        share(n, ALL, ALL)

    @scoped
    def arrive_first(n):
        wait(av.at[n, 0, :, c], aga_r.at[n])
        wait(bv.at[n, :, 0], agb_r.at[n])
        relay(n)
        share(n, LOW, HIGH)

    @scoped
    def arrive_second(n):
        wait(av.at[n, 0, :, c], aga_r.at[n + 1])
        wait(bv.at[n, :, 0], agb_r.at[n + 1])
        share(n, HIGH, LOW)

    def wait_and_sum(n, carry):
        s1_wait(n)
        own_moments(n)
        return carry

    with jax.named_scope("s1_wait"):
        s1_wait(0)
        own(0)
        own_moments(0)
        lax.fori_loop(1, N, wait_and_sum, 0)
    send(ma_mine, ma_in.at[6], ma_s, mo_r.at[4], dev(c_=other))
    with jax.named_scope("mom_0"):
        wait(ma_in.at[6], mo_r.at[4])
    ma_sum[...] = ma_mine[...] + ma_in[6]
    for r, v in enumerate((x1, x2, x3)):
        send(ma_sum, ma_in.at[r], ma_s, mo_r.at[0], dev(x_=v))
    for r, p in enumerate(ys):
        send(mb_mine, mb_in.at[r], mb_s, mo_r.at[1], p)
    own(1)
    arrive(0)
    own(2)
    with jax.named_scope("mom_1"):
        wait(ma_in.at[0:3], mo_r.at[0])
        wait(mb_in.at[0:3], mo_r.at[1])
    ma_all[...] = ma_sum[...] + jnp.sum(ma_in[0:3], 0)
    mb_sum[...] = mb_mine[...] + jnp.sum(mb_in[0:3], 0)
    for r, p in enumerate(zs):
        send(ma_all, ma_in.at[3 + r], ma_s, mo_r.at[2], p)
        send(mb_sum, mb_in.at[3 + r], mb_s, mo_r.at[3], p)
    arrive(1)
    own(3)

    def moments_done():
        with jax.named_scope("mom_2"):
            wait(ma_in.at[3:6], mo_r.at[2])
            wait(mb_in.at[3:6], mo_r.at[3])
        for mine, zin, z0, st, turn in ((ma_all, ma_in, 3, sta, (4, 0, 4)), (mb_sum, mb_in, 3, stb, (0, 4, 4))):
            for n in range(N):
                total = (mine[n] + zin[z0, (n + turn[0]) % N] + zin[z0 + 1, (n + turn[1]) % N]
                         + zin[z0 + 2, (n + turn[2]) % N])
                mean = total[0:1, :] / count
                var = total[1:2, :] / count - mean * mean
                st[n, 0:1, :] = mean
                st[n, 1:2, :] = lax.rsqrt(var + 1e-05)

    @scoped
    def far(n):
        wait(av.at[n, x2, :, c], rla_r.at[n])
        a = av.at[n, x2, :, c]
        send(a, a, a_s, ddf_r.at[n], dev(c_=other))
        wait(bv.at[n, :, y2], rlb_r.at[n])

    def norm_a(n, lo, hi):
        def group(g, carry):
            x0, yh = ring(x2 + 1, lax.div(g, 2)), lax.rem(g, 2)
            at_ = pl.multiple_of((x0 * 2 + yh) * GS, 128)
            for m in range(AW // 128):
                cols = pl.ds(m * 128, 128)
                v = av[n, x0, pl.ds(yh * 2, 2), :, :, cols].reshape(GS, 128).astype(F32)
                v = ((v - sta[n, 0:1, cols]) * sta[n, 1:2, cols]).astype(BF16)
                at[n, cols, pl.ds(at_, GS)] = v.T
            return carry

        lax.fori_loop(lo, hi, group, 0)

    def norm_b(n, lo, hi):
        cols = pl.ds((n % 4) * BW, BW)

        def group(g, carry):
            x0, yh = lax.rem(g, 4), lax.rem(lax.div(y2, 2) + 1 + lax.div(g, 4), 2)
            at_ = pl.multiple_of((x0 * 2 + yh) * GS, 128)
            v = bv[n, x0, pl.ds(yh * 2, 2)].reshape(GS, BW).astype(F32)
            v = ((v - stb[n, 0:1, :]) * stb[n, 1:2, :]).astype(BF16)
            bn[n // 4, pl.ds(at_, GS), cols] = v
            return carry

        lax.fori_loop(lo, hi, group, 0)

    @scoped
    def near_norm(n):
        wait(av.at[n, 0:3, :, other], dd_r.at[n])
        norm_a(n, 0, 6)
        norm_b(n, 0, 4)

    @scoped
    def far_norm_b(n):
        norm_b(n, 4, 8)

    @scoped
    def far_norm_a(n):
        wait(av.at[n, x2, :, other], ddf_r.at[n])
        norm_a(n, 6, 8)

    def dot(i, half, j, n):
        r = jnp.dot(at[i], bn[half, :, j * BW:(j + n) * BW], preferred_element_type=F32)
        return r * (1.0 / count)

    def keep(slot, i, j, v):
        if slot == 1:
            psend[slot, i, j] = encode(v)
        elif slot == 0:
            psend[slot, i, j, 0:128] = encode(v[0:128])
            psend[slot, i, j, 128:256] = encode(v[128:256] + decode(prelay[1, i, j]))
        else:
            psend[slot, i, j, 0:128] = encode(v[0:128] + decode(prelay[0, i, j]))
            psend[slot, i, j, 128:256] = encode(v[128:256])

    def row(slot, m, i, half, n):
        r = dot(i, half, 0, n)
        for j in range(n):
            keep(slot, m, j, r[:, j * BW:(j + 1) * BW])

    def column(slot, m, base, half):
        def one(i, carry):
            keep(slot, i, m, dot(base + i, half, m, 1))
            return carry

        lax.fori_loop(0, m, one, 0)

    def far_wait(m, h):
        wait(bn.at[0, pl.ds(0, 32 * (2 * m + 1))], fr_r.at[m, h])

    def parts(m):
        yield 0, (m, pl.ds(0, m + 1))
        if m:
            yield 1, (pl.ds(0, m), m)

    HALVES = ((0, pl.ds(0, 128)), (1, pl.ds(128, 128)))

    @scoped
    def multiply_far(m):
        for k, cells in parts(m):
            if k:
                column(1, m, 0, 0)
            else:
                row(1, m, m, 0, m + 1)
            for h, rows in HALVES:
                send(psend.at[(1, *cells, rows)], prelay.at[(h, *cells)],
                     z_s, fr_r.at[m, h], (p1, p3)[h])

    def send_1(cells, k):
        send(psend.at[(0, *cells)], precv.at[(0, *cells)], z_s, z1_r.at[k], p1)

    @scoped
    def row_1(n):
        m = n - 4
        if m == 0:
            far_wait(0, 1)
        r = dot(n, 1, 0, m + 1)
        for j in range(m + 1):
            keep(0, m, j, r[:, j * BW:(j + 1) * BW])
            if m == 3:
                send_1((m, j), 1 + j)
        if m < 3:
            send_1((m, pl.ds(0, m + 1)), 0)

    @scoped
    def column_1(n):
        m = n - 4

        if m:
            far_wait(m, 1)

        def one(i, carry):
            keep(0, i, m, dot(4 + i, 1, m, 1))
            if m == 3:
                send_1((i, m), 5 + i)
            return carry

        lax.fori_loop(0, m, one, 0)
        if 0 < m < 3:
            send_1((pl.ds(0, m), m), 0)

    @scoped
    def multiply_3(n):
        m = n - 4
        if m == 0:
            for k in range(4):
                far_wait(k, 0)
            r = held[...]
        else:
            r = dot(n, 0, 0, 4)
        for j in range(4):
            keep(2, m, j, r[:, j * BW:(j + 1) * BW])
            if m == 3:
                send(psend.at[2, m, j], precv.at[1, m, j], z_s, z3_r.at[1 + j], p3)
        if m < 3:
            send(psend.at[2, m], precv.at[1, m], z_s, z3_r.at[0], p3)

    row0 = (zl * 4 + y) * 1024
    col0 = ((x * 2 + zh) * 2 + c) * 512

    def spot(i, j):
        return pl.ds(pl.multiple_of(i * AW, AW), AW), pl.ds(pl.multiple_of(j * BW, BW), BW)

    def add(slot, i, j):
        out_ref[spot(i, j)] = out_ref[spot(i, j)] + decode(precv[slot, i, j])

    def finish(slot, i, j):
        at_ = spot(i, j)
        v = out_ref[at_] + decode(precv[slot, i, j])
        out_ref[at_] = v
        rows = row0 + i * AW + lax.broadcasted_iota(jnp.int32, (AW, BW), 0)
        cols = col0 + j * BW + lax.broadcasted_iota(jnp.int32, (AW, BW), 1)
        term = jnp.where(rows == cols, (1.0 - v) * (1.0 - v), 0.0051 * (v * v))
        lo_sum[...] += jnp.sum(term.reshape(AW // 8, 8, BW), 0)

    lo_sum[...] = jnp.zeros_like(lo_sum)
    moments_done()
    for n in range(1, N - 2):
        if n > 1:
            arrive(n)
            if n + 2 < N - 1:
                own(n + 2)
        near_norm(n - 1)
        far(n - 1)
        far_norm_b(n - 1)
        far_norm_a(n - 1)
        if n < 5:
            multiply_far(n - 1)
        else:
            row_1(4)
            held[...] = dot(4, 0, 0, 4)
    arrive(6)
    own(7)
    near_norm(5)
    far(5)
    multiply_3(4)
    far_norm_b(5)
    column_1(5)
    far_norm_a(5)
    row_1(5)
    near_norm(6)
    far(6)
    far_norm_b(6)
    column_1(6)
    multiply_3(5)
    arrive_first(7)
    far_norm_a(6)
    row_1(6)
    arrive_second(7)
    multiply_3(6)
    near_norm(7)
    far(7)
    far_norm_b(7)
    column_1(7)
    far_norm_a(7)
    row_1(7)
    multiply_3(7)

    with jax.named_scope("mine"):
        def mine(i, carry):
            out_ref[pl.ds(pl.multiple_of(i * AW, AW), AW), :] = dot(i, 1, 0, 4)
            return carry

        lax.fori_loop(0, 4, mine, 0)

    with jax.named_scope("finish_early"):
        wait(precv.at[1, 0:3], z3_r.at[0])

        def adds(t, carry):
            add(1, lax.div(t, 4), lax.rem(t, 4))
            return carry

        lax.fori_loop(0, 12, adds, 0)
        wait(precv.at[0, 0:3, 0:3], z1_r.at[0])

        def early(t, carry):
            finish(0, lax.div(t, 3), lax.rem(t, 3))
            return carry

        lax.fori_loop(0, 9, early, 0)
    with jax.named_scope("finish_late"):
        def late_column(t, carry):
            wait(precv.at[0, t, 3], z1_r.at[5 + t])
            finish(0, t, 3)
            return carry

        def late_row(t, carry):
            wait(precv.at[0, 3, t], z1_r.at[1 + t])
            add(0, 3, t)
            wait(precv.at[1, 3, t], z3_r.at[1 + t])
            finish(1, 3, t)
            return carry

        with jax.named_scope("late_column"):
            lax.fori_loop(0, 3, late_column, 0)
        with jax.named_scope("late_row"):
            lax.fori_loop(0, 4, late_row, 0)

    lo_mine[...] = jnp.sum(lo_sum[...], 0, keepdims=True)
    xs, ys4, cs = (x, x1, x2, x3), (y, y1, y2, y3), (c, other)
    z4 = ((zl, zh), (1 - zl, zh), (zl, 1 - zh), (1 - zl, 1 - zh))
    steps = [(i, j, k, l) for i in range(4) for j in range(4) for k in range(4) for l in range(2)][1:]
    far_first = sorted(steps, key=lambda t: -((0, 1, 2, 1)[t[0]] + (0, 1, 2, 1)[t[1]] + (0, 1, 2, 1)[t[2]]))
    for r, (i, j, k, l) in enumerate(far_first):
        p = dev(x_=xs[i], y_=ys4[j], c_=cs[l], zl_=z4[k][0], zh_=z4[k][1])
        send(lo_mine, lo_in.at[r], lo_s, lo_r, p)
    with jax.named_scope("loss"):
        wait(lo_in, lo_r)
    loss_ref[...] = jnp.sum(lo_mine[...] + jnp.sum(lo_in[...], 0), axis=1, keepdims=True) / width

    with jax.named_scope("drain"):
        wait(a_ref.at[:, 0:6144], s1a_s)
        wait(b_ref.at[:, 0:7168], s1b_s)
        wait(av.at[0:7], a_s)
        wait(bv.at[0:6], b_s)
        wait(psend, z_s)
        wait(ma_in, ma_s)
        wait(mb_in, mb_s)
        wait(lo_in, lo_s)


def shards(view_a, view_b):
    rows, width = view_a.shape
    count = rows * 128
    dma = pltpu.SemaphoreType.DMA
    vm = pltpu.VMEM
    out, loss = pl.pallas_call(
        lambda *refs: kernel(float(count), float(width), *refs),
        out_shape=(pltpu.VMEM((1024, 512), F32), pltpu.VMEM((1, 1), F32)),
        in_specs=[pl.BlockSpec(memory_space=pl.ANY)] * 2,
        out_specs=(pl.BlockSpec(memory_space=pltpu.VMEM), pl.BlockSpec(memory_space=pltpu.VMEM)),
        scratch_shapes=[
            vm((S, width), BF16), vm((S, width), BF16), dma((2,)),
            vm((N, 4, 4, 2, S, AW), BF16),
            vm((N, 4, 4, 2, S, BW), BF16),
            vm((N, AW, K), BF16),
            vm((2, K, 4 * BW), BF16),
            vm((3, 4, 4, AW, BW), BF16),
            vm((2, 4, 4, AW, BW), BF16),
            vm((2, 4, 4, AW // 2, BW), BF16),
            vm((N, 2, AW), F32), vm((7, N, 2, AW), F32), vm((N, 2, AW), F32), vm((N, 2, AW), F32),
            vm((N, 2, BW), F32), vm((6, N, 2, BW), F32), vm((N, 2, BW), F32),
            vm((N, 2, AW), F32), vm((N, 2, BW), F32),
            vm((AW, 4 * BW), F32),
            vm((8, 128), F32), vm((1, 128), F32), vm((127, 1, 128), F32),
            dma, dma((N,)), dma, dma((N,)), dma, dma, dma, dma, dma, dma,
            dma((N + 1,)), dma((N,)), dma((N,)), dma((N,)), dma((N + 1,)), dma((N,)),
            dma((8,)), dma((5,)), dma((4, 2)), dma((5,)), dma,
        ],
        compiler_params=pltpu.CompilerParams(
            collective_id=0, has_side_effects=True, vmem_limit_bytes=59_000_000),
    )(view_a, view_b)
    return out, loss.reshape(())


def solution(mesh):
    finer = Mesh(mesh.devices.reshape(2, 4, 4, 2, 2), ROW_COL)
    in_specs = (P(ROW_COL, None), P(ROW_COL, None))
    out_specs = (P(ROW, COL), P())
    return jax.shard_map(
        shards, mesh=finer, in_specs=in_specs, out_specs=out_specs, check_vma=False
    )
```

```python
import jax
import jax.numpy as jnp
from jax import lax
from jax.experimental import pallas as pl
from jax.experimental.pallas import tpu as pltpu
from jax.sharding import Mesh
from jax.sharding import PartitionSpec as P

ROW = ("row_0", "row_1")
COL = ("col_0", "col_1", "col_2")
ROW_COL = ("row_0", "row_1", "col_0", "col_1", "col_2")

MESH = pl.DeviceIdType.MESH
F32 = jnp.float32
BF16 = jnp.bfloat16

N = 8
S = 96
AW = 256
BW = 128
GS = 384
K = 3072


def encode(v):
    return (v * v * (v * jnp.abs(v))).astype(BF16)


def decode(v):
    v = v.astype(F32)
    root = jnp.sqrt(jnp.sqrt(jnp.abs(v)))
    return jnp.where(v < 0.0, -root, root)


def kernel(count, width, a_hbm, b_hbm, out_ref, loss_ref,
           a_ref, b_ref, in_s, av, bv, at, bn, psend, precv, prelay,
           ma_mine, ma_in, ma_sum, ma_all, mb_mine, mb_in, mb_sum, sta, stb,
           held, lo_sum, lo_mine, lo_in,
           s1a_s, s1b_s, s1_r, a_s, b_s, z_s, ma_s, mb_s, lo_s,
           ag_r, rl_r, dd_r, ddf_r, z1_r, z3_r, fr_r, mo_r, lo_r):
    zl, y, x, zh, c = (lax.axis_index(n) for n in ROW_COL)

    def scoped(f):
        def g(q, *rest):
            with jax.named_scope(f"{f.__name__}_{q}"):
                return f(q, *rest)
        return g

    def dev(x_=None, y_=None, c_=None, zl_=None, zh_=None):
        return (zl if zl_ is None else zl_, y if y_ is None else y_, x if x_ is None else x_,
                zh if zh_ is None else zh_, c if c_ is None else c_)

    def ring(v, d):
        return lax.rem(v + d, 4)

    def xc(r):
        t = lax.rem(x * 2 + c + r, 8)
        return lax.div(t, 2), lax.rem(t, 2)

    def send(src, dst, ss, rs, device):
        pltpu.make_async_remote_copy(src_ref=src, dst_ref=dst, send_sem=ss, recv_sem=rs,
                                     device_id=device, device_id_type=MESH).start()

    def wait(ref, sem):
        pltpu.make_async_copy(ref, ref, sem).wait()

    x1, x2, x3 = ring(x, 1), ring(x, 2), ring(x, 3)
    y1, y2, y3 = ring(y, 1), ring(y, 2), ring(y, 3)
    other = 1 - c
    p1 = dev(zl_=1 - zl)
    p2 = dev(zh_=1 - zh)
    p3 = dev(zl_=1 - zl, zh_=1 - zh)
    xcs = [dev(x_=xc(r)[0], c_=xc(r)[1]) for r in range(1, 8)]
    ys = [dev(y_=v) for v in (y1, y2, y3)]
    zs = [p1, p2, p3]
    load_a = pltpu.make_async_copy(a_hbm, a_ref, in_s.at[0])
    load_b = pltpu.make_async_copy(b_hbm, b_ref, in_s.at[1])
    load_a.start()
    load_b.start()

    barrier = pltpu.get_barrier_semaphore()
    peers = xcs + ys + zs
    with jax.named_scope("barrier"):
        for p in peers:
            pl.semaphore_signal(barrier, inc=1, device_id=p, device_id_type=MESH)
        pl.semaphore_wait(barrier, len(peers))
    load_a.wait()
    load_b.wait()

    def stage1(n, carry):
        k = lax.rem(n, 4)
        ha = lax.rem(zl + lax.div(n, 4), 2)
        hb = lax.rem(zh + 1 + lax.div(n, 4), 2)
        for d in (1, 3, 2, 0):
            yp = ring(y, d)
            cols = pl.ds(pl.multiple_of(ha * 4096 + yp * 1024 + k * AW, AW), AW)
            dst = av.at[n, x, y, c]
            if d:
                send(a_ref.at[:, cols], dst, s1a_s, s1_r.at[n], dev(y_=yp))
            else:
                pltpu.make_async_copy(a_hbm.at[:, cols], dst, s1_r.at[n]).start()
        for r in (1, 2, 3, 7, 6, 5, 4, 0):
            px, pc = xc(r)
            cols = pl.ds(pl.multiple_of(px * 2048 + hb * 1024 + pc * 512 + k * BW, BW), BW)
            dst = bv.at[n, x, y, c]
            if r:
                send(b_ref.at[:, cols], dst, s1b_s, s1_r.at[n], dev(x_=px, c_=pc))
            else:
                pltpu.make_async_copy(b_hbm.at[:, cols], dst, s1_r.at[n]).start()
        return carry

    with jax.named_scope("stage1"):
        lax.fori_loop(0, N, stage1, 0)

    def s1_wait(n):
        wait(av.at[n, 0:2, :, c], s1_r.at[n])

    def own_part(n, up, down, k):
        for part, px, py in ((up, x1, y1), (down, x3, y3)):
            a = av.at[n, x, part, c]
            send(a, a, a_s, ag_r.at[k], dev(x_=px))
            b = bv.at[n, part, y]
            send(b, b, b_s, ag_r.at[k], dev(y_=py))

    ALL, LOW, HIGH = pl.ds(0, 4), pl.ds(0, 2), pl.ds(2, 2)

    @scoped
    def own(n):
        if n < N - 1:
            own_part(n, ALL, ALL, n)
        else:
            own_part(n, LOW, HIGH, n)
            own_part(n, HIGH, LOW, N)
        a = av.at[n, x, :, c]
        send(a, a, a_s, dd_r.at[n], dev(c_=other))

    def own_moments(n):
        def one(k, acc):
            sa, qa, sb, qb = acc
            va = av[n, x, lax.div(k, 2), c, pl.ds(pl.multiple_of(lax.rem(k, 2) * 48, 16), 48), :].astype(F32)
            va = va.reshape(6, 8, AW)
            sa = sa + jnp.sum(va, 0)
            qa = qa + jnp.sum(va * va, 0)
            vb = bv[n, lax.div(k, 2), y, lax.rem(k, 2)].astype(F32).reshape(12, 8, BW)
            sb = sb + jnp.sum(vb, 0)
            qb = qb + jnp.sum(vb * vb, 0)
            return sa, qa, sb, qb

        za, zb = jnp.zeros((8, AW), F32), jnp.zeros((8, BW), F32)
        sa, qa, sb, qb = lax.fori_loop(0, 8, one, (za, za, zb, zb))
        ma_mine[n, 0:1, :] = jnp.sum(sa, 0, keepdims=True)
        ma_mine[n, 1:2, :] = jnp.sum(qa, 0, keepdims=True)
        mb_mine[n, 0:1, :] = jnp.sum(sb, 0, keepdims=True)
        mb_mine[n, 1:2, :] = jnp.sum(qb, 0, keepdims=True)

    def relay(n):
        for v, part, px in ((x3, LOW, x1), (x1, HIGH, x3)):
            a = av.at[n, v, part, c]
            send(a, a, a_s, rl_r.at[n], dev(x_=px))
        for v, part, py in ((y3, LOW, y1), (y1, HIGH, y3)):
            b = bv.at[n, part, v]
            send(b, b, b_s, rl_r.at[n], dev(y_=py))

    def share(n, part3, part1):
        for v, part in ((x3, part3), (x1, part1)):
            a = av.at[n, v, part, c]
            send(a, a, a_s, dd_r.at[n], dev(c_=other))

    @scoped
    def arrive(n):
        wait(av.at[n, :, :, c], ag_r.at[n])
        relay(n)
        share(n, ALL, ALL)

    @scoped
    def arrive_first(n):
        wait(av.at[n, 0:2, :, c], ag_r.at[n])
        relay(n)
        share(n, LOW, HIGH)

    @scoped
    def arrive_second(n):
        wait(av.at[n, 0:2, :, c], ag_r.at[n + 1])
        share(n, HIGH, LOW)

    def wait_and_sum(n, carry):
        s1_wait(n)
        own_moments(n)
        return carry

    with jax.named_scope("s1_wait"):
        s1_wait(0)
        own(0)
        own_moments(0)
        lax.fori_loop(1, N, wait_and_sum, 0)
    send(ma_mine, ma_in.at[6], ma_s, mo_r.at[4], dev(c_=other))
    with jax.named_scope("mom_0"):
        wait(ma_in.at[6], mo_r.at[4])
    ma_sum[...] = ma_mine[...] + ma_in[6]
    for r, v in enumerate((x1, x2, x3)):
        send(ma_sum, ma_in.at[r], ma_s, mo_r.at[0], dev(x_=v))
    for r, p in enumerate(ys):
        send(mb_mine, mb_in.at[r], mb_s, mo_r.at[1], p)
    own(1)
    arrive(0)
    own(2)
    with jax.named_scope("mom_1"):
        wait(ma_in.at[0:3], mo_r.at[0])
        wait(mb_in.at[0:3], mo_r.at[1])
    ma_all[...] = ma_sum[...] + jnp.sum(ma_in[0:3], 0)
    mb_sum[...] = mb_mine[...] + jnp.sum(mb_in[0:3], 0)
    for r, p in enumerate(zs):
        send(ma_all, ma_in.at[3 + r], ma_s, mo_r.at[2], p)
        send(mb_sum, mb_in.at[3 + r], mb_s, mo_r.at[3], p)
    arrive(1)
    own(3)

    def moments_done():
        with jax.named_scope("mom_2"):
            wait(ma_in.at[3:6], mo_r.at[2])
            wait(mb_in.at[3:6], mo_r.at[3])
        for mine, zin, z0, st, turn in ((ma_all, ma_in, 3, sta, (4, 0, 4)), (mb_sum, mb_in, 3, stb, (0, 4, 4))):
            for n in range(N):
                total = (mine[n] + zin[z0, (n + turn[0]) % N] + zin[z0 + 1, (n + turn[1]) % N]
                         + zin[z0 + 2, (n + turn[2]) % N])
                mean = total[0:1, :] / count
                var = total[1:2, :] / count - mean * mean
                st[n, 0:1, :] = mean
                st[n, 1:2, :] = lax.rsqrt(var + 1e-05)

    @scoped
    def far(n):
        wait(av.at[n, 0:2, :, c], rl_r.at[n])
        a = av.at[n, x2, :, c]
        send(a, a, a_s, ddf_r.at[n], dev(c_=other))

    def norm_a(n, lo, hi):
        def group(g, carry):
            x0, yh = ring(x2 + 1, lax.div(g, 2)), lax.rem(g, 2)
            at_ = pl.multiple_of((x0 * 2 + yh) * GS, 128)
            for m in range(AW // 128):
                cols = pl.ds(m * 128, 128)
                v = av[n, x0, pl.ds(yh * 2, 2), :, :, cols].reshape(GS, 128).astype(F32)
                v = ((v - sta[n, 0:1, cols]) * sta[n, 1:2, cols]).astype(BF16)
                at[n, cols, pl.ds(at_, GS)] = v.T
            return carry

        lax.fori_loop(lo, hi, group, 0)

    def norm_b(n, lo, hi):
        cols = pl.ds((n % 4) * BW, BW)

        def group(g, carry):
            x0, yh = lax.rem(g, 4), lax.rem(lax.div(y2, 2) + 1 + lax.div(g, 4), 2)
            at_ = pl.multiple_of((x0 * 2 + yh) * GS, 128)
            v = bv[n, x0, pl.ds(yh * 2, 2)].reshape(GS, BW).astype(F32)
            v = ((v - stb[n, 0:1, :]) * stb[n, 1:2, :]).astype(BF16)
            bn[n // 4, pl.ds(at_, GS), cols] = v
            return carry

        lax.fori_loop(lo, hi, group, 0)

    @scoped
    def near_norm(n):
        wait(av.at[n, 0:3, :, other], dd_r.at[n])
        norm_a(n, 0, 6)
        norm_b(n, 0, 4)

    @scoped
    def far_norm_b(n):
        norm_b(n, 4, 8)

    @scoped
    def far_norm_a(n):
        wait(av.at[n, x2, :, other], ddf_r.at[n])
        norm_a(n, 6, 8)

    def dot(i, half, j, n):
        r = jnp.dot(at[i], bn[half, :, j * BW:(j + n) * BW], preferred_element_type=F32)
        return r * (1.0 / count)

    def keep(slot, i, j, v):
        if slot == 1:
            psend[slot, i, j] = encode(v)
        elif slot == 0:
            psend[slot, i, j, 0:128] = encode(v[0:128])
            psend[slot, i, j, 128:256] = encode(v[128:256] + decode(prelay[1, i, j]))
        else:
            psend[slot, i, j, 0:128] = encode(v[0:128] + decode(prelay[0, i, j]))
            psend[slot, i, j, 128:256] = encode(v[128:256])

    def row(slot, m, i, half, n):
        r = dot(i, half, 0, n)
        for j in range(n):
            keep(slot, m, j, r[:, j * BW:(j + 1) * BW])

    def column(slot, m, base, half):
        def one(i, carry):
            keep(slot, i, m, dot(base + i, half, m, 1))
            return carry

        lax.fori_loop(0, m, one, 0)

    def far_wait(m, h):
        wait(bn.at[0, pl.ds(0, 32 * (2 * m + 1))], fr_r.at[m, h])

    def parts(m):
        yield 0, (m, pl.ds(0, m + 1))
        if m:
            yield 1, (pl.ds(0, m), m)

    HALVES = ((0, pl.ds(0, 128)), (1, pl.ds(128, 128)))

    @scoped
    def multiply_far(m):
        for k, cells in parts(m):
            if k:
                column(1, m, 0, 0)
            else:
                row(1, m, m, 0, m + 1)
            for h, rows in HALVES:
                send(psend.at[(1, *cells, rows)], prelay.at[(h, *cells)],
                     z_s, fr_r.at[m, h], (p1, p3)[h])

    def send_1(cells, k):
        send(psend.at[(0, *cells)], precv.at[(0, *cells)], z_s, z1_r.at[k], p1)

    @scoped
    def row_1(n):
        m = n - 4
        if m == 0:
            far_wait(0, 1)
        r = dot(n, 1, 0, m + 1)
        for j in range(m + 1):
            keep(0, m, j, r[:, j * BW:(j + 1) * BW])
            if m == 3:
                send_1((m, j), 1 + j)
        if m < 3:
            send_1((m, pl.ds(0, m + 1)), 0)

    @scoped
    def column_1(n):
        m = n - 4

        if m:
            far_wait(m, 1)

        def one(i, carry):
            keep(0, i, m, dot(4 + i, 1, m, 1))
            if m == 3:
                send_1((i, m), 5 + i)
            return carry

        lax.fori_loop(0, m, one, 0)
        if 0 < m < 3:
            send_1((pl.ds(0, m), m), 0)

    @scoped
    def multiply_3(n):
        m = n - 4
        if m == 0:
            for k in range(4):
                far_wait(k, 0)
            r = held[...]
        else:
            r = dot(n, 0, 0, 4)
        for j in range(4):
            keep(2, m, j, r[:, j * BW:(j + 1) * BW])
            if m == 3:
                send(psend.at[2, m, j], precv.at[1, m, j], z_s, z3_r.at[1 + j], p3)
        if m < 3:
            send(psend.at[2, m], precv.at[1, m], z_s, z3_r.at[0], p3)

    row0 = (zl * 4 + y) * 1024
    col0 = ((x * 2 + zh) * 2 + c) * 512

    def spot(i, j):
        return pl.ds(pl.multiple_of(i * AW, AW), AW), pl.ds(pl.multiple_of(j * BW, BW), BW)

    def add(slot, i, j):
        out_ref[spot(i, j)] = out_ref[spot(i, j)] + decode(precv[slot, i, j])

    def finish(slot, i, j):
        at_ = spot(i, j)
        v = out_ref[at_] + decode(precv[slot, i, j])
        out_ref[at_] = v
        rows = row0 + i * AW + lax.broadcasted_iota(jnp.int32, (AW, BW), 0)
        cols = col0 + j * BW + lax.broadcasted_iota(jnp.int32, (AW, BW), 1)
        term = jnp.where(rows == cols, (1.0 - v) * (1.0 - v), 0.0051 * (v * v))
        lo_sum[...] += jnp.sum(term.reshape(AW // 8, 8, BW), 0)

    lo_sum[...] = jnp.zeros_like(lo_sum)
    moments_done()
    for n in range(1, N - 2):
        if n > 1:
            arrive(n)
            if n + 2 < N - 1:
                own(n + 2)
        near_norm(n - 1)
        far(n - 1)
        far_norm_b(n - 1)
        far_norm_a(n - 1)
        if n < 5:
            multiply_far(n - 1)
        else:
            row_1(4)
            held[...] = dot(4, 0, 0, 4)
    arrive(6)
    own(7)
    near_norm(5)
    far(5)
    multiply_3(4)
    far_norm_b(5)
    column_1(5)
    far_norm_a(5)
    row_1(5)
    near_norm(6)
    far(6)
    far_norm_b(6)
    column_1(6)
    multiply_3(5)
    arrive_first(7)
    far_norm_a(6)
    row_1(6)
    arrive_second(7)
    multiply_3(6)
    near_norm(7)
    far(7)
    far_norm_b(7)
    column_1(7)
    far_norm_a(7)
    row_1(7)
    multiply_3(7)

    with jax.named_scope("mine"):
        def mine(i, carry):
            out_ref[pl.ds(pl.multiple_of(i * AW, AW), AW), :] = dot(i, 1, 0, 4)
            return carry

        lax.fori_loop(0, 4, mine, 0)

    with jax.named_scope("finish_early"):
        wait(precv.at[1, 0:3], z3_r.at[0])

        def adds(t, carry):
            add(1, lax.div(t, 4), lax.rem(t, 4))
            return carry

        lax.fori_loop(0, 12, adds, 0)
        wait(precv.at[0, 0:3, 0:3], z1_r.at[0])

        def early(t, carry):
            finish(0, lax.div(t, 3), lax.rem(t, 3))
            return carry

        lax.fori_loop(0, 9, early, 0)
    with jax.named_scope("finish_late"):
        def late_column(t, carry):
            wait(precv.at[0, t, 3], z1_r.at[5 + t])
            finish(0, t, 3)
            return carry

        def late_row(t, carry):
            wait(precv.at[0, 3, t], z1_r.at[1 + t])
            add(0, 3, t)
            wait(precv.at[1, 3, t], z3_r.at[1 + t])
            finish(1, 3, t)
            return carry

        with jax.named_scope("late_column"):
            lax.fori_loop(0, 3, late_column, 0)
        with jax.named_scope("late_row"):
            lax.fori_loop(0, 4, late_row, 0)

    lo_mine[...] = jnp.sum(lo_sum[...], 0, keepdims=True)
    xs, ys4, cs = (x, x1, x2, x3), (y, y1, y2, y3), (c, other)
    z4 = ((zl, zh), (1 - zl, zh), (zl, 1 - zh), (1 - zl, 1 - zh))
    steps = [(i, j, k, l) for i in range(4) for j in range(4) for k in range(4) for l in range(2)][1:]
    far_first = sorted(steps, key=lambda t: -((0, 1, 2, 1)[t[0]] + (0, 1, 2, 1)[t[1]] + (0, 1, 2, 1)[t[2]]))
    for r, (i, j, k, l) in enumerate(far_first):
        p = dev(x_=xs[i], y_=ys4[j], c_=cs[l], zl_=z4[k][0], zh_=z4[k][1])
        send(lo_mine, lo_in.at[r], lo_s, lo_r, p)
    with jax.named_scope("loss"):
        wait(lo_in, lo_r)
    loss_ref[...] = jnp.sum(lo_mine[...] + jnp.sum(lo_in[...], 0), axis=1, keepdims=True) / width

    with jax.named_scope("drain"):
        wait(a_ref.at[:, 0:6144], s1a_s)
        wait(b_ref.at[:, 0:7168], s1b_s)
        wait(av.at[0:7], a_s)
        wait(bv.at[0:6], b_s)
        wait(psend, z_s)
        wait(ma_in, ma_s)
        wait(mb_in, mb_s)
        wait(lo_in, lo_s)


def shards(view_a, view_b):
    rows, width = view_a.shape
    count = rows * 128
    dma = pltpu.SemaphoreType.DMA
    vm = pltpu.VMEM
    out, loss = pl.pallas_call(
        lambda *refs: kernel(float(count), float(width), *refs),
        out_shape=(pltpu.VMEM((1024, 512), F32), pltpu.VMEM((1, 1), F32)),
        in_specs=[pl.BlockSpec(memory_space=pl.ANY)] * 2,
        out_specs=(pl.BlockSpec(memory_space=pltpu.VMEM), pl.BlockSpec(memory_space=pltpu.VMEM)),
        scratch_shapes=[
            vm((S, width), BF16), vm((S, width), BF16), dma((2,)),
            vm((N, 4, 4, 2, S, AW), BF16),
            vm((N, 4, 4, 2, S, BW), BF16),
            vm((N, AW, K), BF16),
            vm((2, K, 4 * BW), BF16),
            vm((3, 4, 4, AW, BW), BF16),
            vm((2, 4, 4, AW, BW), BF16),
            vm((2, 4, 4, AW // 2, BW), BF16),
            vm((N, 2, AW), F32), vm((7, N, 2, AW), F32), vm((N, 2, AW), F32), vm((N, 2, AW), F32),
            vm((N, 2, BW), F32), vm((6, N, 2, BW), F32), vm((N, 2, BW), F32),
            vm((N, 2, AW), F32), vm((N, 2, BW), F32),
            vm((AW, 4 * BW), F32),
            vm((8, 128), F32), vm((1, 128), F32), vm((127, 1, 128), F32),
            dma, dma, dma((N,)), dma, dma, dma, dma, dma, dma,
            dma((N + 1,)), dma((N,)), dma((N,)), dma((N,)),
            dma((8,)), dma((5,)), dma((4, 2)), dma((5,)), dma,
        ],
        compiler_params=pltpu.CompilerParams(
            collective_id=0, has_side_effects=True, vmem_limit_bytes=59_000_000),
    )(view_a, view_b)
    return out, loss.reshape(())


def solution(mesh):
    finer = Mesh(mesh.devices.reshape(2, 4, 4, 2, 2), ROW_COL)
    in_specs = (P(ROW_COL, None), P(ROW_COL, None))
    out_specs = (P(ROW, COL), P())
    return jax.shard_map(
        shards, mesh=finer, in_specs=in_specs, out_specs=out_specs, check_vma=False
    )
```
